512 devices in a mesh: chan: 16 (over x_hi, z), tm: 8 (over y), row: 4 (over x_lo, core).
Axes of the slice: x: 4 (x_hi: 2, x_lo: 2; x = x_hi * 2 + x_lo), y: 8, z: 8, core: 2. Of those that a mesh axis runs over, the one named last changes fastest.
Arguments:
- samples: bfloat16 [32, 4096, 4096], P(('tm', 'row'), None, 'chan'), may hold values from -6 to 6
- channel_index: int32 [16], replicated, may hold values from 1 to 2047
- gain_real: float32 [16, 4096], P(None, 'chan'), may hold values from -4 to 4
- gain_imag: float32 [16, 4096], P(None, 'chan'), may hold values from -4 to 4
- flags: int32 [2048], P('chan'), may hold values 0 or 1
Outputs:
- visibility: bfloat16 [2, 16, 4096, 4096], P(None, 'chan', 'row', 'tm')
The draws below stay inside these ranges and needn't reach their ends.
Inputs may be any that keep to these rules, and one draw needn't show every extreme that they name: `channel_index`: channel numbers, not necessarily distinct.
All inputs are finite; a program needn't handle non-finite values. No bound on the sum of `flags` on one device may be relied on, other than what follows from the above.
Results may differ from the reference program's by a relative error of at most 0.0056.
Values may be sent and summed in bfloat16 or wider, within the bound.
A program may use at most 64 MiB of HBM per device.

```python
import math
import jax
import jax.numpy as jnp
from jax import lax

P_SIZE = 4096
TAPS = 4
INPUTS = 4096
CHANNELS = 16
ANTENNAS = 2048
FRAMES = 32


def place_ends(values, rng, low, high):
    index_at = [jax.random.randint(jax.random.fold_in(rng, axis), (), 0, length) for axis, length in enumerate(values.shape)]
    longest = values.shape.index(max(values.shape))
    beside = index_at[:longest] + [(index_at[longest] + 1) % values.shape[longest]] + index_at[longest + 1:]
    return values.at[tuple(index_at)].set(low).at[tuple(beside)].set(high)


def block_levels(own_key, shape, cuts, smallest, largest):
    def one(axis_at, shards_of):
        draws = jax.random.uniform(jax.random.fold_in(jax.random.fold_in(own_key, 6), axis_at), (shards_of,), jnp.float32, smallest / len(cuts), largest / len(cuts))
        return jnp.repeat(jnp.exp(draws), shape[axis_at] // shards_of).reshape((-1,) + (1,) * (len(shape) - axis_at - 1))

    level = one(*cuts[0])
    for cut in cuts[1:]:
        level = level * one(*cut)
    return level


def normal_values(own_key, shape, scale, most, pieces=(), kind=jnp.bfloat16):
    values = jax.random.normal(own_key, shape, jnp.float32) * scale
    if len(pieces) > 0:
        values = block_levels(own_key, shape, pieces, -0.22, 0.18) * values
    return jnp.clip(values, min=-most, max=most).astype(kind)


def setup_inputs(seed: int = 0) -> dict:
    key_of = jax.random.split(jax.random.key(seed), 6)
    return {
        "samples": normal_values(key_of[0], (FRAMES, P_SIZE, INPUTS), 1.0, 6.0, ((0, 32), (2, 16))),
        "channel_index": place_ends(jax.random.randint(key_of[1], (CHANNELS,), 1, P_SIZE // 2), jax.random.fold_in(key_of[1], 1), 1, (P_SIZE // 2) - 1).astype(jnp.int32),
        "gain_real": normal_values(key_of[2], (CHANNELS, INPUTS), 0.7, 4.0, ((1, 16),), jnp.float32),
        "gain_imag": normal_values(key_of[3], (CHANNELS, INPUTS), 0.7, 4.0, ((1, 16),), jnp.float32),
        "flags": place_ends((jax.random.randint(key_of[4], (ANTENNAS,), 0, 8) < 7).astype(jnp.int32), jax.random.fold_in(key_of[4], 1), 0, 1),
    }


def filter_taps():
    sample_index = jnp.arange(TAPS * P_SIZE, dtype=jnp.int32).astype(jnp.float32)
    centered = (sample_index + 0.5 - TAPS * P_SIZE / 2) / P_SIZE
    hann_taper = 0.5 - 0.5 * jnp.cos(2.0 * math.pi * (sample_index + 0.5) / (TAPS * P_SIZE))
    return (jnp.sinc(centered) * hann_taper).reshape(TAPS, P_SIZE)

def dft_table(channel_index):
    points = jnp.arange(P_SIZE, dtype=jnp.int32)
    phase_index = channel_index[:, None] * points[None, :] % P_SIZE
    angles = 2.0 * math.pi * phase_index.astype(jnp.float32) / P_SIZE
    scale = 1.0 / math.sqrt(P_SIZE)
    return jnp.concatenate([jnp.cos(angles) * scale, -jnp.sin(angles) * scale], 0)

def reference(samples, channel_index, gain_real, gain_imag, flags):
    filters = filter_taps()
    table = dft_table(channel_index)
    padded = jnp.concatenate([jnp.zeros((TAPS - 1, P_SIZE, INPUTS), jnp.bfloat16), samples], 0)

    def one_frame(frame):
        window = lax.dynamic_slice_in_dim(padded, frame, TAPS, 0).astype(jnp.float32)
        weighted = lax.optimization_barrier(jnp.sum(filters[:, :, None] * window, 0))
        return jnp.dot(table, weighted, precision=lax.Precision.HIGHEST)
    spectra = lax.map(one_frame, jnp.arange(FRAMES, dtype=jnp.int32))
    spec_re = spectra[:, :CHANNELS]
    spec_im = spectra[:, CHANNELS:]
    usable = jnp.repeat(flags, 2).astype(jnp.float32)
    volt_re = (usable * (gain_real * spec_re - gain_imag * spec_im)).astype(jnp.bfloat16)
    volt_im = (usable * (gain_real * spec_im + gain_imag * spec_re)).astype(jnp.bfloat16)

    def one_channel(pair):
        real_part, imag_part = pair
        left_side = jnp.concatenate([real_part, imag_part], 0)
        right_side = jnp.concatenate([jnp.concatenate([real_part, -imag_part], 1), jnp.concatenate([imag_part, real_part], 1)], 0)
        product = lax.dot_general(left_side, right_side, (((0,), (0,)), ((), ())), preferred_element_type=jnp.float32)
        result = jnp.stack([product[:, :INPUTS], product[:, INPUTS:]], 0) / FRAMES
        return result.astype(jnp.bfloat16)
    per_channel = lax.map(one_channel, (volt_re.transpose(1, 0, 2), volt_im.transpose(1, 0, 2)))
    return per_channel.transpose(1, 0, 2, 3)
```

```python
import functools
import math

import jax
import jax.numpy as jnp
import numpy as np
from jax import lax
from jax.experimental import pallas as pl
from jax.experimental.pallas import tpu as pltpu
from jax.sharding import PartitionSpec as P

P_SIZE = 4096
TAPS = 4
CHANNELS = 16
N_CHAN, N_TM, N_ROW = 16, 8, 4
N_FRAMES = N_TM * N_ROW
BLOCK = 256
CHUNK = 512
MESH = pl.DeviceIdType.MESH
F32, BF16 = jnp.float32, jnp.bfloat16


def filter_taps():
    at = np.arange(TAPS * P_SIZE, dtype=np.float64) + 0.5
    centered = (at - TAPS * P_SIZE / 2) / P_SIZE
    taper = 0.5 - 0.5 * np.cos(2.0 * math.pi * at / (TAPS * P_SIZE))
    return (np.sinc(centered) * taper).reshape(TAPS, P_SIZE).astype(np.float32)


def cos_sin(phase):
    quarter = lax.shift_right_logical(phase + 512, 10)
    rest = phase - lax.shift_left(quarter, 10)
    x = rest.astype(F32) * (2.0 * math.pi / P_SIZE)
    y = x * x
    s = x + x * y * (-1 / 6 + y * (1 / 120 + y * (-1 / 5040 + y * (1 / 362880))))
    c = 1.0 + y * (-0.5 + y * (1 / 24 + y * (-1 / 720 + y * (1 / 40320))))
    odd = (quarter & 1) == 1
    cos = jnp.where(odd, s, c)
    sin = jnp.where(odd, c, s)
    cos = jnp.where(((quarter + 1) & 2) == 2, -cos, cos)
    sin = jnp.where((quarter & 2) == 2, -sin, sin)
    return cos, sin


def far_first(i):
    half = (i + 1) // 2
    return 4 + half * (1 - 2 * (i % 2))


def gather_kernel(
    x_hbm, ci_hbm, filt_hbm, gr_hbm, gi_hbm, flags_hbm,
    rows_out, cols_out,
    x, ci, filt, gr, gi, flags, lhs, send, parts, volts,
    local_sems, send_sem1, send_sem2, parts_sems, rows_sem, cols_sem,
):
    me_c = lax.axis_index("chan")
    me_t = lax.axis_index("tm")
    me_r = lax.axis_index("row")
    frame = me_t * N_ROW + me_r

    loads = [
        pltpu.make_async_copy(src, dst, local_sems.at[i])
        for i, (src, dst) in enumerate(
            [(ci_hbm, ci), (filt_hbm, filt), (gr_hbm, gr), (gi_hbm, gi),
             (flags_hbm, flags), (x_hbm.at[0], x)]
        )
    ]
    for copy in loads:
        copy.start()

    barrier = pltpu.get_barrier_semaphore()

    def greet_chan(i, _):
        peer = (me_c + i) % N_CHAN
        for back in range(TAPS):
            @pl.when(frame >= back)
            def _():
                other = frame - back
                pl.semaphore_signal(
                    barrier, inc=1,
                    device_id=(peer, other // N_ROW, other % N_ROW), device_id_type=MESH,
                )
        return 0

    lax.fori_loop(1, N_CHAN, greet_chan, 0)

    def greet_frames(i, _):
        other = (frame + i) % N_FRAMES
        pl.semaphore_signal(
            barrier, inc=1,
            device_id=(me_c, other // N_ROW, other % N_ROW), device_id_type=MESH,
        )
        return 0

    lax.fori_loop(1, N_FRAMES, greet_frames, 0)

    for before in range(1, TAPS):
        @pl.when(frame < before)
        def _():
            parts[TAPS - 1 - before] = jnp.zeros(parts.shape[1:], F32)

    loads[0].wait()
    loads[1].wait()
    row_of = lax.broadcasted_iota(jnp.int32, (CHANNELS, CHUNK), 0)
    chan_at = jnp.zeros((CHANNELS, CHUNK), jnp.int32)
    for c in range(CHANNELS):
        chan_at = jnp.where(row_of == c, ci[c], chan_at)
    lane = lax.broadcasted_iota(jnp.int32, (CHANNELS, CHUNK), 1)

    def one_chunk(n, _):
        at = pl.ds(pl.multiple_of(n * CHUNK, CHUNK), CHUNK)
        phase = (chan_at * (lane + n * CHUNK)) & (P_SIZE - 1)
        cos, sin = cos_sin(phase)
        scale = 1.0 / math.sqrt(P_SIZE)
        table = (cos * scale, sin * -scale)
        for k in range(TAPS):
            tap = filt[k : k + 1, at]
            for part in range(2):
                value = table[part] * tap
                high = value.astype(BF16)
                low = (value - high.astype(F32)).astype(BF16)
                row = (2 * k + part) * CHANNELS
                lhs[row : row + CHANNELS, at] = high
                lhs[row + 128 : row + 128 + CHANNELS, at] = low
        return 0

    lax.fori_loop(0, P_SIZE // CHUNK, one_chunk, 0)

    for copy in loads[2:]:
        copy.wait()
    both = jnp.dot(lhs[...], x[...], preferred_element_type=F32)
    spectra = both[:128] + both[128:]

    twice = (
        lax.broadcasted_iota(jnp.int32, (128, BLOCK), 1) // 2
        == lax.broadcasted_iota(jnp.int32, (128, BLOCK), 0)
    ).astype(BF16)
    alive = jnp.dot(
        jnp.broadcast_to(flags[...].astype(F32), (CHANNELS, 128)).astype(BF16), twice,
        preferred_element_type=F32,
    )
    real_gain = gr[...] * alive
    imag_gain = gi[...] * alive
    planes = []
    for k in range(TAPS):
        s_re = spectra[32 * k : 32 * k + 16]
        s_im = spectra[32 * k + 16 : 32 * k + 32]
        planes += [real_gain * s_re - imag_gain * s_im, real_gain * s_im + imag_gain * s_re]
    planes = jnp.concatenate(planes, 0)
    to = lax.broadcasted_iota(jnp.int32, (128, 128), 0)
    source = (to % 8) * 16 + to // 8
    turn = (lax.broadcasted_iota(jnp.int32, (128, 128), 1) == source).astype(F32)
    turned = jnp.dot(
        turn, planes, precision=lax.Precision.HIGHEST, preferred_element_type=F32
    )
    send[...] = turned.reshape(64, 2, BLOCK)

    ahead_count = jnp.minimum(N_FRAMES - 1 - frame, TAPS - 1)
    pl.semaphore_wait(barrier, (N_CHAN - 1) * (1 + ahead_count) + N_FRAMES - 1)

    def part_copy(c, ahead):
        k = TAPS - 1 - ahead
        other = frame + ahead
        return pltpu.make_async_remote_copy(
            src_ref=send.at[c * TAPS + k],
            dst_ref=parts.at[k, me_c],
            send_sem=send_sem1.at[k],
            recv_sem=parts_sems.at[k],
            device_id=(c, other // N_ROW, other % N_ROW),
            device_id_type=MESH,
        )

    def send_parts(i, _):
        z = (me_c % 8 + far_first(i % 8)) % 8
        half = (me_c // 8 + 1 + i // 8) % 2
        c = half * 8 + z
        for ahead in range(TAPS - 1, 0, -1):
            @pl.when(frame + ahead < N_FRAMES)
            def _():
                part_copy(c, ahead).start()

        @pl.when(i < N_CHAN - 1)
        def _():
            part_copy(c, 0).start()
        return 0

    parts[TAPS - 1, me_c] = send[me_c * TAPS + TAPS - 1]
    lax.fori_loop(0, N_CHAN, send_parts, 0)

    for k in range(TAPS - 1):
        @pl.when(frame >= TAPS - 1 - k)
        def _():
            pltpu.make_async_copy(parts.at[k], parts.at[k], parts_sems.at[k]).wait()
    own = parts.at[TAPS - 1, pl.ds(0, N_CHAN - 1)]
    pltpu.make_async_copy(own, own, parts_sems.at[TAPS - 1]).wait()

    volts[...] = (((parts[0] + parts[1]) + parts[2]) + parts[3]).astype(BF16)

    def volt_copies(t, r):
        rows = pltpu.make_async_remote_copy(
            src_ref=volts.at[pl.ds(r * 4, 4)],
            dst_ref=rows_out.at[frame],
            send_sem=send_sem2.at[0],
            recv_sem=rows_sem,
            device_id=(me_c, t, r),
            device_id_type=MESH,
        )
        cols = pltpu.make_async_remote_copy(
            src_ref=volts.at[pl.ds(t * 2, 2)],
            dst_ref=cols_out.at[frame],
            send_sem=send_sem2.at[1],
            recv_sem=cols_sem,
            device_id=(me_c, t, r),
            device_id_type=MESH,
        )
        return rows, cols

    def send_volts(i, _):
        t = (me_t + far_first(i // 4)) % N_TM
        r = (me_r + 1 + i % 4) % N_ROW
        rows, cols = volt_copies(t, r)
        rows.start()
        cols.start()
        return 0

    rows_out[frame] = volts[pl.ds(me_r * 4, 4)]
    cols_out[frame] = volts[pl.ds(me_t * 2, 2)]
    lax.fori_loop(0, N_FRAMES - 1, send_volts, 0)

    for ref, sem in ((rows_out, rows_sem), (cols_out, cols_sem)):
        others = ref.at[pl.ds(0, N_FRAMES - 1)]
        pltpu.make_async_copy(others, others, sem).wait()

    for k in range(TAPS - 1):
        @pl.when(frame + TAPS - 1 - k < N_FRAMES)
        def _():
            pltpu.make_async_copy(parts.at[k], parts.at[k], send_sem1.at[k]).wait()
    pltpu.make_async_copy(own, own, send_sem1.at[TAPS - 1]).wait()
    for ref, at in ((rows_out, 0), (cols_out, 1)):
        others = ref.at[pl.ds(0, N_FRAMES - 1)]
        pltpu.make_async_copy(others, others, send_sem2.at[at]).wait()


def correlate_kernel(rows, cols, out, right):
    @pl.when(pl.program_id(0) == 0)
    def _():
        to = lax.broadcasted_iota(jnp.int32, (64, 64), 0)
        at = lax.broadcasted_iota(jnp.int32, (64, 64), 1)
        sign = jnp.where(to % 2 == 0, -1.0, 1.0)
        swap = jnp.where(at == to + 1 - 2 * (to % 2), sign, 0.0).astype(BF16)
        panel = jnp.concatenate([cols[:, 0].reshape(64, BLOCK), cols[:, 1].reshape(64, BLOCK)], 1)
        right[:, :512] = panel
        right[:, 512:] = jnp.dot(swap, panel, preferred_element_type=F32).astype(BF16)

    left = rows[:, pl.program_id(0)].reshape(64, BLOCK)
    product = lax.dot_general(
        left, right[...], (((0,), (0,)), ((), ())), preferred_element_type=F32
    )
    product = product * (1.0 / N_FRAMES)
    out[0, 0] = product[:, :512].astype(BF16)
    out[1, 0] = product[:, 512:].astype(BF16)


def local(samples, channel_index, gain_real, gain_imag, flags):
    anywhere = pl.BlockSpec(memory_space=pl.ANY)
    vmem = pl.BlockSpec(memory_space=pltpu.VMEM)
    rows, cols = pl.pallas_call(
        gather_kernel,
        out_shape=(
            jax.ShapeDtypeStruct((N_FRAMES, 4, 2, BLOCK), BF16),
            jax.ShapeDtypeStruct((N_FRAMES, 2, 2, BLOCK), BF16),
        ),
        in_specs=[anywhere] * 6,
        out_specs=(vmem, vmem),
        scratch_shapes=[
            pltpu.VMEM((P_SIZE, BLOCK), BF16),
            pltpu.SMEM((CHANNELS,), jnp.int32),
            pltpu.VMEM((TAPS, P_SIZE), F32),
            pltpu.VMEM((CHANNELS, BLOCK), F32),
            pltpu.VMEM((CHANNELS, BLOCK), F32),
            pltpu.VMEM((1, 128), jnp.int32),
            pltpu.VMEM((256, P_SIZE), BF16),
            pltpu.VMEM((CHANNELS * TAPS, 2, BLOCK), F32),
            pltpu.VMEM((TAPS, N_CHAN, 2, BLOCK), F32),
            pltpu.VMEM((N_CHAN, 2, BLOCK), BF16),
            pltpu.SemaphoreType.DMA((6,)),
            pltpu.SemaphoreType.DMA((TAPS,)),
            pltpu.SemaphoreType.DMA((2,)),
            pltpu.SemaphoreType.DMA((TAPS,)),
            pltpu.SemaphoreType.DMA,
            pltpu.SemaphoreType.DMA,
        ],
        compiler_params=pltpu.CompilerParams(
            collective_id=0, has_side_effects=True, vmem_limit_bytes=16 * 2**20
        ),
        name="spectra_and_gather",
    )(samples, channel_index, jnp.asarray(filter_taps()), gain_real, gain_imag,
      flags.reshape(1, 128))
    return pl.pallas_call(
        correlate_kernel,
        grid=(4,),
        out_shape=jax.ShapeDtypeStruct((2, 1, 1024, 512), BF16),
        in_specs=[vmem, vmem],
        out_specs=pl.BlockSpec((2, 1, BLOCK, 512), lambda i: (0, 0, i, 0)),
        scratch_shapes=[pltpu.VMEM((64, 1024), BF16)],
        compiler_params=pltpu.CompilerParams(vmem_limit_bytes=16 * 2**20),
        name="correlate",
    )(rows, cols)


def solution(mesh):
    in_specs = (P(("tm", "row"), None, "chan"), P(), P(None, "chan"), P(None, "chan"), P("chan"))
    out_specs = P(None, "chan", "row", "tm")
    return jax.shard_map(local, mesh=mesh, in_specs=in_specs, out_specs=out_specs, check_vma=False)
```

```python
import functools
import math

import jax
import jax.numpy as jnp
import numpy as np
from jax import lax
from jax.experimental import pallas as pl
from jax.experimental.pallas import tpu as pltpu
from jax.sharding import PartitionSpec as P

P_SIZE = 4096
TAPS = 4
CHANNELS = 16
N_CHAN, N_TM, N_ROW = 16, 8, 4
N_FRAMES = N_TM * N_ROW
BLOCK = 256
CHUNK = 512
MESH = pl.DeviceIdType.MESH
F32, BF16 = jnp.float32, jnp.bfloat16


def filter_taps():
    at = np.arange(TAPS * P_SIZE, dtype=np.float64) + 0.5
    centered = (at - TAPS * P_SIZE / 2) / P_SIZE
    taper = 0.5 - 0.5 * np.cos(2.0 * math.pi * at / (TAPS * P_SIZE))
    return (np.sinc(centered) * taper).reshape(TAPS, P_SIZE).astype(np.float32)


def cos_sin(phase):
    quarter = lax.shift_right_logical(phase + 512, 10)
    rest = phase - lax.shift_left(quarter, 10)
    x = rest.astype(F32) * (2.0 * math.pi / P_SIZE)
    y = x * x
    s = x + x * y * (-1 / 6 + y * (1 / 120 + y * (-1 / 5040 + y * (1 / 362880))))
    c = 1.0 + y * (-0.5 + y * (1 / 24 + y * (-1 / 720 + y * (1 / 40320))))
    odd = (quarter & 1) == 1
    cos = jnp.where(odd, s, c)
    sin = jnp.where(odd, c, s)
    cos = jnp.where(((quarter + 1) & 2) == 2, -cos, cos)
    sin = jnp.where((quarter & 2) == 2, -sin, sin)
    return cos, sin


def far_first(i):
    half = (i + 1) // 2
    return 4 + half * (1 - 2 * (i % 2))


def gather_kernel(
    x_hbm, ci_hbm, filt_hbm, gr_hbm, gi_hbm, flags_hbm,
    rows_out, cols_out,
    x, ci, filt, gr, gi, flags, lhs, send, parts, volts,
    local_sems, send_sem1, send_sem2, parts_sems, rows_sem, cols_sem,
):
    me_c = lax.axis_index("chan")
    me_t = lax.axis_index("tm")
    me_r = lax.axis_index("row")
    frame = me_t * N_ROW + me_r

    loads = [
        pltpu.make_async_copy(src, dst, local_sems.at[i])
        for i, (src, dst) in enumerate(
            [(ci_hbm, ci), (filt_hbm, filt), (gr_hbm, gr), (gi_hbm, gi),
             (flags_hbm, flags), (x_hbm.at[0], x)]
        )
    ]
    for copy in loads:
        copy.start()

    barrier = pltpu.get_barrier_semaphore()

    def greet_chan(i, _):
        peer = (me_c + i) % N_CHAN
        for back in range(TAPS):
            @pl.when(frame >= back)
            def _():
                other = frame - back
                pl.semaphore_signal(
                    barrier, inc=1,
                    device_id=(peer, other // N_ROW, other % N_ROW), device_id_type=MESH,
                )
        return 0

    lax.fori_loop(1, N_CHAN, greet_chan, 0)

    def greet_frames(i, _):
        other = (frame + i) % N_FRAMES
        pl.semaphore_signal(
            barrier, inc=1,
            device_id=(me_c, other // N_ROW, other % N_ROW), device_id_type=MESH,
        )
        return 0

    lax.fori_loop(1, N_FRAMES, greet_frames, 0)

    for before in range(1, TAPS):
        @pl.when(frame < before)
        def _():
            parts[TAPS - 1 - before] = jnp.zeros(parts.shape[1:], F32)

    loads[0].wait()
    loads[1].wait()
    row_of = lax.broadcasted_iota(jnp.int32, (CHANNELS, CHUNK), 0)
    chan_at = jnp.zeros((CHANNELS, CHUNK), jnp.int32)
    for c in range(CHANNELS):
        chan_at = jnp.where(row_of == c, ci[c], chan_at)
    lane = lax.broadcasted_iota(jnp.int32, (CHANNELS, CHUNK), 1)

    def one_chunk(n, _):
        at = pl.ds(pl.multiple_of(n * CHUNK, CHUNK), CHUNK)
        phase = (chan_at * (lane + n * CHUNK)) & (P_SIZE - 1)
        cos, sin = cos_sin(phase)
        scale = 1.0 / math.sqrt(P_SIZE)
        table = (cos * scale, sin * -scale)
        for k in range(TAPS):
            tap = filt[k : k + 1, at]
            for part in range(2):
                value = table[part] * tap
                high = value.astype(BF16)
                low = (value - high.astype(F32)).astype(BF16)
                row = (2 * k + part) * CHANNELS
                lhs[row : row + CHANNELS, at] = high
                lhs[row + 128 : row + 128 + CHANNELS, at] = low
        return 0

    lax.fori_loop(0, P_SIZE // CHUNK, one_chunk, 0)

    for copy in loads[2:]:
        copy.wait()
    both = jnp.dot(lhs[...], x[...], preferred_element_type=F32)
    spectra = both[:128] + both[128:]

    twice = (
        lax.broadcasted_iota(jnp.int32, (128, BLOCK), 1) // 2
        == lax.broadcasted_iota(jnp.int32, (128, BLOCK), 0)
    ).astype(BF16)
    alive = jnp.dot(
        jnp.broadcast_to(flags[...].astype(F32), (CHANNELS, 128)).astype(BF16), twice,
        preferred_element_type=F32,
    )
    real_gain = gr[...] * alive
    imag_gain = gi[...] * alive
    planes = []
    for k in range(TAPS):
        s_re = spectra[32 * k : 32 * k + 16]
        s_im = spectra[32 * k + 16 : 32 * k + 32]
        planes += [real_gain * s_re - imag_gain * s_im, real_gain * s_im + imag_gain * s_re]
    planes = jnp.concatenate(planes, 0)
    to = lax.broadcasted_iota(jnp.int32, (128, 128), 0)
    source = (to % 8) * 16 + to // 8
    turn = (lax.broadcasted_iota(jnp.int32, (128, 128), 1) == source).astype(F32)
    turned = jnp.dot(
        turn, planes, precision=lax.Precision.HIGHEST, preferred_element_type=F32
    )
    send[...] = turned.reshape(64, 2, BLOCK)

    ahead_count = jnp.minimum(N_FRAMES - 1 - frame, TAPS - 1)
    pl.semaphore_wait(barrier, (N_CHAN - 1) * (1 + ahead_count) + N_FRAMES - 1)

    def part_copy(c, ahead):
        k = TAPS - 1 - ahead
        other = frame + ahead
        return pltpu.make_async_remote_copy(
            src_ref=send.at[c * TAPS + k],
            dst_ref=parts.at[k, me_c],
            send_sem=send_sem1.at[k],
            recv_sem=parts_sems.at[k],
            device_id=(c, other // N_ROW, other % N_ROW),
            device_id_type=MESH,
        )

    def send_parts(i, _):
        z = (me_c % 8 + far_first(i % 8)) % 8
        half = (me_c // 8 + 1 + i // 8) % 2
        c = half * 8 + z
        for ahead in range(TAPS - 1, 0, -1):
            @pl.when(frame + ahead < N_FRAMES)
            def _():
                part_copy(c, ahead).start()

        @pl.when(i < N_CHAN - 1)
        def _():
            part_copy(c, 0).start()
        return 0

    parts[TAPS - 1, me_c] = send[me_c * TAPS + TAPS - 1]
    lax.fori_loop(0, N_CHAN, send_parts, 0)

    for k in range(TAPS - 1):
        @pl.when(frame >= TAPS - 1 - k)
        def _():
            pltpu.make_async_copy(parts.at[k], parts.at[k], parts_sems.at[k]).wait()
    own = parts.at[TAPS - 1, pl.ds(0, N_CHAN - 1)]
    pltpu.make_async_copy(own, own, parts_sems.at[TAPS - 1]).wait()

    volts[...] = (((parts[0] + parts[1]) + parts[2]) + parts[3]).astype(BF16)

    def volt_copies(t, r):
        rows = pltpu.make_async_remote_copy(
            src_ref=volts.at[pl.ds(r * 4, 4)],
            dst_ref=rows_out.at[frame],
            send_sem=send_sem2.at[0],
            recv_sem=rows_sem,
            device_id=(me_c, t, r),
            device_id_type=MESH,
        )
        cols = pltpu.make_async_remote_copy(
            src_ref=volts.at[pl.ds(t * 2, 2)],
            dst_ref=cols_out.at[frame],
            send_sem=send_sem2.at[1],
            recv_sem=cols_sem,
            device_id=(me_c, t, r),
            device_id_type=MESH,
        )
        return rows, cols

    def send_volts(i, _):
        t = (me_t + far_first(i // 4)) % N_TM
        r = (me_r + 1 + i % 4) % N_ROW
        rows, cols = volt_copies(t, r)
        rows.start()
        cols.start()
        return 0

    rows_out[frame] = volts[pl.ds(me_r * 4, 4)]
    cols_out[frame] = volts[pl.ds(me_t * 2, 2)]
    lax.fori_loop(0, N_FRAMES - 1, send_volts, 0)

    for ref, sem in ((rows_out, rows_sem), (cols_out, cols_sem)):
        others = ref.at[pl.ds(0, N_FRAMES - 1)]
        pltpu.make_async_copy(others, others, sem).wait()

    for k in range(TAPS - 1):
        @pl.when(frame + TAPS - 1 - k < N_FRAMES)
        def _():
            pltpu.make_async_copy(parts.at[k], parts.at[k], send_sem1.at[k]).wait()
    pltpu.make_async_copy(own, own, send_sem1.at[TAPS - 1]).wait()
    for ref, at in ((rows_out, 0), (cols_out, 1)):
        others = ref.at[pl.ds(0, N_FRAMES - 1)]
        pltpu.make_async_copy(others, others, send_sem2.at[at]).wait()


def correlate_kernel(rows, cols, out, right):
    @pl.when(pl.program_id(0) == 0)
    def _():
        to = lax.broadcasted_iota(jnp.int32, (64, 64), 0)
        at = lax.broadcasted_iota(jnp.int32, (64, 64), 1)
        sign = jnp.where(to % 2 == 0, -1.0, 1.0)
        swap = jnp.where(at == to + 1 - 2 * (to % 2), sign, 0.0).astype(BF16)
        panel = jnp.concatenate([cols[:, 0].reshape(64, BLOCK), cols[:, 1].reshape(64, BLOCK)], 1)
        right[:, :512] = panel
        right[:, 512:] = jnp.dot(swap, panel, preferred_element_type=F32).astype(BF16)

    left = rows[:, pl.program_id(0)].reshape(64, BLOCK)
    product = lax.dot_general(
        left, right[...], (((0,), (0,)), ((), ())), preferred_element_type=F32
    )
    product = product * (1.0 / N_FRAMES)
    out[0, 0] = product[:, :512].astype(BF16)
    out[1, 0] = product[:, 512:].astype(BF16)


def local(samples, channel_index, gain_real, gain_imag, flags):
    in_hbm = pl.BlockSpec(memory_space=pltpu.HBM)
    vmem = pl.BlockSpec(memory_space=pltpu.VMEM)
    rows, cols = pl.pallas_call(
        gather_kernel,
        out_shape=(
            jax.ShapeDtypeStruct((N_FRAMES, 4, 2, BLOCK), BF16),
            jax.ShapeDtypeStruct((N_FRAMES, 2, 2, BLOCK), BF16),
        ),
        in_specs=[in_hbm] * 6,
        out_specs=(vmem, vmem),
        scratch_shapes=[
            pltpu.VMEM((P_SIZE, BLOCK), BF16),
            pltpu.SMEM((CHANNELS,), jnp.int32),
            pltpu.VMEM((TAPS, P_SIZE), F32),
            pltpu.VMEM((CHANNELS, BLOCK), F32),
            pltpu.VMEM((CHANNELS, BLOCK), F32),
            pltpu.VMEM((1, 128), jnp.int32),
            pltpu.VMEM((256, P_SIZE), BF16),
            pltpu.VMEM((CHANNELS * TAPS, 2, BLOCK), F32),
            pltpu.VMEM((TAPS, N_CHAN, 2, BLOCK), F32),
            pltpu.VMEM((N_CHAN, 2, BLOCK), BF16),
            pltpu.SemaphoreType.DMA((6,)),
            pltpu.SemaphoreType.DMA((TAPS,)),
            pltpu.SemaphoreType.DMA((2,)),
            pltpu.SemaphoreType.DMA((TAPS,)),
            pltpu.SemaphoreType.DMA,
            pltpu.SemaphoreType.DMA,
        ],
        compiler_params=pltpu.CompilerParams(
            collective_id=0, has_side_effects=True, vmem_limit_bytes=16 * 2**20
        ),
        name="spectra_and_gather",
    )(*[
        pltpu.with_memory_space_constraint(value, pltpu.HBM)
        for value in (samples, channel_index, jnp.asarray(filter_taps()), gain_real, gain_imag,
                      flags.reshape(1, 128))
    ])
    return pl.pallas_call(
        correlate_kernel,
        grid=(4,),
        out_shape=jax.ShapeDtypeStruct((2, 1, 1024, 512), BF16),
        in_specs=[vmem, vmem],
        out_specs=pl.BlockSpec((2, 1, BLOCK, 512), lambda i: (0, 0, i, 0)),
        scratch_shapes=[pltpu.VMEM((64, 1024), BF16)],
        compiler_params=pltpu.CompilerParams(vmem_limit_bytes=16 * 2**20),
        name="correlate",
    )(rows, cols)


def solution(mesh):
    in_specs = (P(("tm", "row"), None, "chan"), P(), P(None, "chan"), P(None, "chan"), P("chan"))
    out_specs = P(None, "chan", "row", "tm")
    return jax.shard_map(local, mesh=mesh, in_specs=in_specs, out_specs=out_specs, check_vma=False)
```

```python
import functools
import math

import jax
import jax.numpy as jnp
import numpy as np
from jax import lax
from jax.experimental import pallas as pl
from jax.experimental.pallas import tpu as pltpu
from jax.sharding import PartitionSpec as P

P_SIZE = 4096
TAPS = 4
CHANNELS = 16
N_CHAN, N_TM, N_ROW = 16, 8, 4
N_FRAMES = N_TM * N_ROW
BLOCK = 256
CHUNK = 512
MESH = pl.DeviceIdType.MESH
F32, BF16 = jnp.float32, jnp.bfloat16


def filter_taps():
    at = np.arange(TAPS * P_SIZE, dtype=np.float64) + 0.5
    centered = (at - TAPS * P_SIZE / 2) / P_SIZE
    taper = 0.5 - 0.5 * np.cos(2.0 * math.pi * at / (TAPS * P_SIZE))
    return (np.sinc(centered) * taper).reshape(TAPS, P_SIZE).astype(np.float32)


def cos_sin(phase):
    quarter = lax.shift_right_logical(phase + 512, 10)
    rest = phase - lax.shift_left(quarter, 10)
    x = rest.astype(F32) * (2.0 * math.pi / P_SIZE)
    y = x * x
    s = x + x * y * (-1 / 6 + y * (1 / 120 + y * (-1 / 5040 + y * (1 / 362880))))
    c = 1.0 + y * (-0.5 + y * (1 / 24 + y * (-1 / 720 + y * (1 / 40320))))
    odd = (quarter & 1) == 1
    cos = jnp.where(odd, s, c)
    sin = jnp.where(odd, c, s)
    cos = jnp.where(((quarter + 1) & 2) == 2, -cos, cos)
    sin = jnp.where((quarter & 2) == 2, -sin, sin)
    return cos, sin


FAR_FIRST = (4, 3, 5, 2, 6, 1, 7, 0)


def gather_kernel(
    x_hbm, ci_hbm, filt_hbm, gr_hbm, gi_hbm, flags_hbm,
    rows_out, cols_out,
    x, ci, filt, gr, gi, flags, lhs, send, parts, volts,
    local_sems, send_sem1, send_sem2, parts_sems, rows_sem, cols_sem,
):
    me_c = lax.axis_index("chan")
    me_t = lax.axis_index("tm")
    me_r = lax.axis_index("row")
    frame = me_t * N_ROW + me_r
    z_at = [lax.rem(lax.rem(me_c, 8) + step, 8) for step in FAR_FIRST]
    half_at = [lax.rem(lax.div(me_c, 8) + step, 2) * 8 for step in (1, 0)]
    chans = [half + z for z in z_at for half in half_at]
    tms = [lax.rem(me_t + step, N_TM) for step in FAR_FIRST]
    rows_at = [lax.rem(me_r + step, N_ROW) for step in (2, 3, 1, 0)]
    group = [(t, r) for t in tms for r in rows_at][:-1]

    def place(number):
        return lax.div(number, N_ROW), lax.rem(number, N_ROW)

    barrier = pltpu.get_barrier_semaphore()

    def greet(c, t, r):
        pl.semaphore_signal(barrier, inc=1, device_id=(c, t, r), device_id_type=MESH)

    for back in range(TAPS - 1, 0, -1):
        @pl.when(frame >= back)
        def _():
            for c in chans[:-1]:
                greet(c, *place(frame - back))

    for c in chans[:-1]:
        greet(c, me_t, me_r)
    for t, r in group:
        greet(me_c, t, r)

    loads = [
        pltpu.make_async_copy(src, dst, local_sems.at[i])
        for i, (src, dst) in enumerate(
            [(ci_hbm, ci), (filt_hbm, filt), (gr_hbm, gr), (gi_hbm, gi),
             (flags_hbm, flags), (x_hbm.at[0], x)]
        )
    ]
    for copy in loads:
        copy.start()

    for before in range(1, TAPS):
        @pl.when(frame < before)
        def _():
            parts[TAPS - 1 - before] = jnp.zeros(parts.shape[1:], F32)

    loads[0].wait()
    loads[1].wait()
    row_of = lax.broadcasted_iota(jnp.int32, (CHANNELS, CHUNK), 0)
    chan_at = jnp.zeros((CHANNELS, CHUNK), jnp.int32)
    for c in range(CHANNELS):
        chan_at = jnp.where(row_of == c, ci[c], chan_at)
    lane = lax.broadcasted_iota(jnp.int32, (CHANNELS, CHUNK), 1)

    def one_chunk(n, _):
        at = pl.ds(pl.multiple_of(n * CHUNK, CHUNK), CHUNK)
        phase = (chan_at * (lane + n * CHUNK)) & (P_SIZE - 1)
        cos, sin = cos_sin(phase)
        scale = 1.0 / math.sqrt(P_SIZE)
        table = (cos * scale, sin * -scale)
        for k in range(TAPS):
            tap = filt[k : k + 1, at]
            for part in range(2):
                value = table[part] * tap
                high = value.astype(BF16)
                low = (value - high.astype(F32)).astype(BF16)
                row = (2 * k + part) * CHANNELS
                lhs[row : row + CHANNELS, at] = high
                lhs[row + 128 : row + 128 + CHANNELS, at] = low
        return 0

    lax.fori_loop(0, P_SIZE // CHUNK, one_chunk, 0)

    for copy in loads[2:]:
        copy.wait()
    both = jnp.dot(lhs[...], x[...], preferred_element_type=F32)
    spectra = both[:128] + both[128:]

    twice = (
        lax.broadcasted_iota(jnp.int32, (128, BLOCK), 1) // 2
        == lax.broadcasted_iota(jnp.int32, (128, BLOCK), 0)
    ).astype(BF16)
    alive = jnp.dot(
        jnp.broadcast_to(flags[...].astype(F32), (CHANNELS, 128)).astype(BF16), twice,
        preferred_element_type=F32,
    )
    real_gain = gr[...] * alive
    imag_gain = gi[...] * alive
    planes = []
    for k in range(TAPS):
        s_re = spectra[32 * k : 32 * k + 16]
        s_im = spectra[32 * k + 16 : 32 * k + 32]
        planes += [real_gain * s_re - imag_gain * s_im, real_gain * s_im + imag_gain * s_re]
    planes = jnp.concatenate(planes, 0)
    to = lax.broadcasted_iota(jnp.int32, (128, 128), 0)
    source = (to % 8) * 16 + to // 8
    turn = (lax.broadcasted_iota(jnp.int32, (128, 128), 1) == source).astype(F32)
    turned = jnp.dot(
        turn, planes, precision=lax.Precision.HIGHEST, preferred_element_type=F32
    )
    send[...] = turned.reshape(64, 2, BLOCK)

    ahead_count = jnp.minimum(N_FRAMES - 1 - frame, TAPS - 1)
    pl.semaphore_wait(barrier, (N_CHAN - 1) * (1 + ahead_count) + N_FRAMES - 1)

    def send_part(c, ahead):
        k = TAPS - 1 - ahead
        pltpu.make_async_remote_copy(
            src_ref=send.at[c * TAPS + k],
            dst_ref=parts.at[k, me_c],
            send_sem=send_sem1.at[k],
            recv_sem=parts_sems.at[k],
            device_id=(c, *place(frame + ahead)),
            device_id_type=MESH,
        ).start()

    for ahead in range(TAPS - 1, 0, -1):
        @pl.when(frame + ahead < N_FRAMES)
        def _():
            for c in chans:
                send_part(c, ahead)

    for c in chans[:-1]:
        send_part(c, 0)
    parts[TAPS - 1, me_c] = send[me_c * TAPS + TAPS - 1]

    for k in range(TAPS - 1):
        @pl.when(frame >= TAPS - 1 - k)
        def _():
            pltpu.make_async_copy(parts.at[k], parts.at[k], parts_sems.at[k]).wait()
    own = parts.at[TAPS - 1, pl.ds(0, N_CHAN - 1)]
    pltpu.make_async_copy(own, own, parts_sems.at[TAPS - 1]).wait()

    volts[...] = (((parts[0] + parts[1]) + parts[2]) + parts[3]).astype(BF16)

    for t, r in group:
        for src, dst, at, sem in (
            (volts.at[pl.ds(r * 4, 4)], rows_out, 0, rows_sem),
            (volts.at[pl.ds(t * 2, 2)], cols_out, 1, cols_sem),
        ):
            pltpu.make_async_remote_copy(
                src_ref=src,
                dst_ref=dst.at[frame],
                send_sem=send_sem2.at[at],
                recv_sem=sem,
                device_id=(me_c, t, r),
                device_id_type=MESH,
            ).start()
    rows_out[frame] = volts[pl.ds(me_r * 4, 4)]
    cols_out[frame] = volts[pl.ds(me_t * 2, 2)]

    for ref, sem in ((rows_out, rows_sem), (cols_out, cols_sem)):
        others = ref.at[pl.ds(0, N_FRAMES - 1)]
        pltpu.make_async_copy(others, others, sem).wait()

    for k in range(TAPS - 1):
        @pl.when(frame + TAPS - 1 - k < N_FRAMES)
        def _():
            pltpu.make_async_copy(parts.at[k], parts.at[k], send_sem1.at[k]).wait()
    pltpu.make_async_copy(own, own, send_sem1.at[TAPS - 1]).wait()
    for ref, at in ((rows_out, 0), (cols_out, 1)):
        others = ref.at[pl.ds(0, N_FRAMES - 1)]
        pltpu.make_async_copy(others, others, send_sem2.at[at]).wait()


def correlate_kernel(rows, cols, out, right):
    @pl.when(pl.program_id(0) == 0)
    def _():
        to = lax.broadcasted_iota(jnp.int32, (64, 64), 0)
        at = lax.broadcasted_iota(jnp.int32, (64, 64), 1)
        sign = jnp.where(to % 2 == 0, -1.0, 1.0)
        swap = jnp.where(at == to + 1 - 2 * (to % 2), sign, 0.0).astype(BF16)
        panel = jnp.concatenate([cols[:, 0].reshape(64, BLOCK), cols[:, 1].reshape(64, BLOCK)], 1)
        right[:, :512] = panel
        right[:, 512:] = jnp.dot(swap, panel, preferred_element_type=F32).astype(BF16)

    left = rows[:, pl.program_id(0)].reshape(64, BLOCK)
    product = lax.dot_general(
        left, right[...], (((0,), (0,)), ((), ())), preferred_element_type=F32
    )
    product = product * (1.0 / N_FRAMES)
    out[0, 0] = product[:, :512].astype(BF16)
    out[1, 0] = product[:, 512:].astype(BF16)


def local(samples, channel_index, gain_real, gain_imag, flags):
    in_hbm = pl.BlockSpec(memory_space=pltpu.HBM)
    vmem = pl.BlockSpec(memory_space=pltpu.VMEM)
    rows, cols = pl.pallas_call(
        gather_kernel,
        out_shape=(
            jax.ShapeDtypeStruct((N_FRAMES, 4, 2, BLOCK), BF16),
            jax.ShapeDtypeStruct((N_FRAMES, 2, 2, BLOCK), BF16),
        ),
        in_specs=[in_hbm] * 6,
        out_specs=(vmem, vmem),
        scratch_shapes=[
            pltpu.VMEM((P_SIZE, BLOCK), BF16),
            pltpu.SMEM((CHANNELS,), jnp.int32),
            pltpu.VMEM((TAPS, P_SIZE), F32),
            pltpu.VMEM((CHANNELS, BLOCK), F32),
            pltpu.VMEM((CHANNELS, BLOCK), F32),
            pltpu.VMEM((1, 128), jnp.int32),
            pltpu.VMEM((256, P_SIZE), BF16),
            pltpu.VMEM((CHANNELS * TAPS, 2, BLOCK), F32),
            pltpu.VMEM((TAPS, N_CHAN, 2, BLOCK), F32),
            pltpu.VMEM((N_CHAN, 2, BLOCK), BF16),
            pltpu.SemaphoreType.DMA((6,)),
            pltpu.SemaphoreType.DMA((TAPS,)),
            pltpu.SemaphoreType.DMA((2,)),
            pltpu.SemaphoreType.DMA((TAPS,)),
            pltpu.SemaphoreType.DMA,
            pltpu.SemaphoreType.DMA,
        ],
        compiler_params=pltpu.CompilerParams(
            collective_id=0, has_side_effects=True, vmem_limit_bytes=16 * 2**20
        ),
        name="spectra_and_gather",
    )(*[
        pltpu.with_memory_space_constraint(value, pltpu.HBM)
        for value in (samples, channel_index, jnp.asarray(filter_taps()), gain_real, gain_imag,
                      flags.reshape(1, 128))
    ])
    return pl.pallas_call(
        correlate_kernel,
        grid=(4,),
        out_shape=jax.ShapeDtypeStruct((2, 1, 1024, 512), BF16),
        in_specs=[vmem, vmem],
        out_specs=pl.BlockSpec((2, 1, BLOCK, 512), lambda i: (0, 0, i, 0)),
        scratch_shapes=[pltpu.VMEM((64, 1024), BF16)],
        compiler_params=pltpu.CompilerParams(vmem_limit_bytes=16 * 2**20),
        name="correlate",
    )(rows, cols)


def solution(mesh):
    in_specs = (P(("tm", "row"), None, "chan"), P(), P(None, "chan"), P(None, "chan"), P("chan"))
    out_specs = P(None, "chan", "row", "tm")
    return jax.shard_map(local, mesh=mesh, in_specs=in_specs, out_specs=out_specs, check_vma=False)
```

```python
import functools
import math

import jax
import jax.numpy as jnp
import numpy as np
from jax import lax
from jax.experimental import pallas as pl
from jax.experimental.pallas import tpu as pltpu
from jax.sharding import PartitionSpec as P

P_SIZE = 4096
TAPS = 4
CHANNELS = 16
N_CHAN, N_TM, N_ROW = 16, 8, 4
N_FRAMES = N_TM * N_ROW
BLOCK = 256
CHUNK = 512
STRIP, STRIPS = 128, 8
MESH = pl.DeviceIdType.MESH
F32, BF16 = jnp.float32, jnp.bfloat16


def filter_taps():
    at = np.arange(TAPS * P_SIZE, dtype=np.float64) + 0.5
    centered = (at - TAPS * P_SIZE / 2) / P_SIZE
    taper = 0.5 - 0.5 * np.cos(2.0 * math.pi * at / (TAPS * P_SIZE))
    return (np.sinc(centered) * taper).reshape(TAPS, P_SIZE).astype(np.float32)


def cos_sin(phase):
    quarter = lax.shift_right_logical(phase + 512, 10)
    rest = phase - lax.shift_left(quarter, 10)
    x = rest.astype(F32) * (2.0 * math.pi / P_SIZE)
    y = x * x
    s = x + x * y * (-1 / 6 + y * (1 / 120 + y * (-1 / 5040 + y * (1 / 362880))))
    c = 1.0 + y * (-0.5 + y * (1 / 24 + y * (-1 / 720 + y * (1 / 40320))))
    odd = (quarter & 1) == 1
    cos = jnp.where(odd, s, c)
    sin = jnp.where(odd, c, s)
    cos = jnp.where(((quarter + 1) & 2) == 2, -cos, cos)
    sin = jnp.where((quarter & 2) == 2, -sin, sin)
    return cos, sin


FAR_FIRST = (4, 3, 5, 2, 6, 1, 7, 0)


def gather_kernel(
    x_hbm, ci_hbm, filt_hbm, gr_hbm, gi_hbm, flags_hbm,
    rows_out, cols_out,
    x, ci, filt, gr, gi, flags, lhs, send, parts, volts,
    local_sems, send_sem1, send_sem2, parts_sems, rows_sem, cols_sem,
):
    me_c = lax.axis_index("chan")
    me_t = lax.axis_index("tm")
    me_r = lax.axis_index("row")
    frame = me_t * N_ROW + me_r
    z_at = [lax.rem(lax.rem(me_c, 8) + step, 8) for step in FAR_FIRST]
    half_at = [lax.rem(lax.div(me_c, 8) + step, 2) * 8 for step in (1, 0)]
    chans = [half + z for z in z_at for half in half_at]
    tms = [lax.rem(me_t + step, N_TM) for step in FAR_FIRST]
    rows_at = [lax.rem(me_r + step, N_ROW) for step in (2, 3, 1, 0)]
    group = [(t, r) for t in tms for r in rows_at][:-1]

    def place(number):
        return lax.div(number, N_ROW), lax.rem(number, N_ROW)

    barrier = pltpu.get_barrier_semaphore()

    def greet(c, t, r):
        pl.semaphore_signal(barrier, inc=1, device_id=(c, t, r), device_id_type=MESH)

    for back in range(TAPS - 1, 0, -1):
        @pl.when(frame >= back)
        def _():
            for c in chans[:-1]:
                greet(c, *place(frame - back))

    for c in chans[:-1]:
        greet(c, me_t, me_r)
    for t, r in group:
        greet(me_c, t, r)

    loads = [
        pltpu.make_async_copy(src, dst, local_sems.at[i])
        for i, (src, dst) in enumerate(
            [(ci_hbm, ci), (filt_hbm, filt), (gr_hbm, gr), (gi_hbm, gi),
             (flags_hbm, flags), (x_hbm.at[0], x)]
        )
    ]
    for copy in loads:
        copy.start()

    for before in range(1, TAPS):
        @pl.when(frame < before)
        def _():
            parts[TAPS - 1 - before] = jnp.zeros(parts.shape[1:], F32)

    loads[0].wait()
    loads[1].wait()
    row_of = lax.broadcasted_iota(jnp.int32, (CHANNELS, CHUNK), 0)
    chan_at = jnp.zeros((CHANNELS, CHUNK), jnp.int32)
    for c in range(CHANNELS):
        chan_at = jnp.where(row_of == c, ci[c], chan_at)
    lane = lax.broadcasted_iota(jnp.int32, (CHANNELS, CHUNK), 1)

    def one_chunk(n, _):
        at = pl.ds(pl.multiple_of(n * CHUNK, CHUNK), CHUNK)
        phase = (chan_at * (lane + n * CHUNK)) & (P_SIZE - 1)
        cos, sin = cos_sin(phase)
        scale = 1.0 / math.sqrt(P_SIZE)
        table = (cos * scale, sin * -scale)
        for k in range(TAPS):
            tap = filt[k : k + 1, at]
            for part in range(2):
                value = table[part] * tap
                high = value.astype(BF16)
                low = (value - high.astype(F32)).astype(BF16)
                row = (2 * k + part) * CHANNELS
                lhs[row : row + CHANNELS, at] = high
                lhs[row + 128 : row + 128 + CHANNELS, at] = low
        return 0

    lax.fori_loop(0, P_SIZE // CHUNK, one_chunk, 0)

    for copy in loads[2:]:
        copy.wait()
    both = jnp.dot(lhs[...], x[...], preferred_element_type=F32)
    spectra = both[:128] + both[128:]

    twice = (
        lax.broadcasted_iota(jnp.int32, (128, BLOCK), 1) // 2
        == lax.broadcasted_iota(jnp.int32, (128, BLOCK), 0)
    ).astype(BF16)
    alive = jnp.dot(
        jnp.broadcast_to(flags[...].astype(F32), (CHANNELS, 128)).astype(BF16), twice,
        preferred_element_type=F32,
    )
    real_gain = gr[...] * alive
    imag_gain = gi[...] * alive
    planes = []
    for k in range(TAPS):
        s_re = spectra[32 * k : 32 * k + 16]
        s_im = spectra[32 * k + 16 : 32 * k + 32]
        planes += [real_gain * s_re - imag_gain * s_im, real_gain * s_im + imag_gain * s_re]
    planes = jnp.concatenate(planes, 0)
    to = lax.broadcasted_iota(jnp.int32, (128, 128), 0)
    source = (to % 8) * 16 + to // 8
    turn = (lax.broadcasted_iota(jnp.int32, (128, 128), 1) == source).astype(F32)
    turned = jnp.dot(
        turn, planes, precision=lax.Precision.HIGHEST, preferred_element_type=F32
    )
    send[...] = turned.reshape(64, 2, BLOCK)

    ahead_count = jnp.minimum(N_FRAMES - 1 - frame, TAPS - 1)
    pl.semaphore_wait(barrier, (N_CHAN - 1) * (1 + ahead_count) + N_FRAMES - 1)

    def send_part(c, ahead):
        k = TAPS - 1 - ahead
        pltpu.make_async_remote_copy(
            src_ref=send.at[c * TAPS + k],
            dst_ref=parts.at[k, me_c],
            send_sem=send_sem1.at[k],
            recv_sem=parts_sems.at[k],
            device_id=(c, *place(frame + ahead)),
            device_id_type=MESH,
        ).start()

    for z in range(8):
        for ahead in range(TAPS - 1, 0, -1):
            @pl.when(frame + ahead < N_FRAMES)
            def _():
                for half in (0, 8):
                    send_part(half + z, ahead)

        for half in (0, 8):
            @pl.when(me_c != half + z)
            def _():
                send_part(half + z, 0)
    parts[TAPS - 1, me_c] = send[me_c * TAPS + TAPS - 1]

    for k in range(TAPS - 1):
        @pl.when(frame >= TAPS - 1 - k)
        def _():
            pltpu.make_async_copy(parts.at[k], parts.at[k], parts_sems.at[k]).wait()
    own = parts.at[TAPS - 1, pl.ds(0, N_CHAN - 1)]
    pltpu.make_async_copy(own, own, parts_sems.at[TAPS - 1]).wait()

    volts[...] = (((parts[0] + parts[1]) + parts[2]) + parts[3]).astype(BF16)

    def send_volts(t, r):
        for src, dst, at, sem in (
            (volts.at[pl.ds(r * 4, 4)], rows_out, 0, rows_sem),
            (volts.at[pl.ds(t * 2, 2)], cols_out, 1, cols_sem),
        ):
            pltpu.make_async_remote_copy(
                src_ref=src,
                dst_ref=dst.at[frame],
                send_sem=send_sem2.at[at],
                recv_sem=sem,
                device_id=(me_c, t, r),
                device_id_type=MESH,
            ).start()

    for t in (0, 1, 7, 2, 6, 3, 5, 4):
        for r in (1, 3, 2, 0):
            @pl.when(frame != t * N_ROW + r)
            def _():
                send_volts(t, r)

    rows_out[frame] = volts[pl.ds(me_r * 4, 4)]
    cols_out[frame] = volts[pl.ds(me_t * 2, 2)]

    for ref, sem in ((rows_out, rows_sem), (cols_out, cols_sem)):
        others = ref.at[pl.ds(0, N_FRAMES - 1)]
        pltpu.make_async_copy(others, others, sem).wait()

    for k in range(TAPS - 1):
        @pl.when(frame + TAPS - 1 - k < N_FRAMES)
        def _():
            pltpu.make_async_copy(parts.at[k], parts.at[k], send_sem1.at[k]).wait()
    pltpu.make_async_copy(own, own, send_sem1.at[TAPS - 1]).wait()
    for ref, at in ((rows_out, 0), (cols_out, 1)):
        others = ref.at[pl.ds(0, N_FRAMES - 1)]
        pltpu.make_async_copy(others, others, send_sem2.at[at]).wait()


def correlate_kernel(rows, cols, out_hbm, right, out, sems):
    to = lax.broadcasted_iota(jnp.int32, (64, 64), 0)
    at = lax.broadcasted_iota(jnp.int32, (64, 64), 1)
    sign = jnp.where(to % 2 == 0, -1.0, 1.0)
    swap = jnp.where(at == to + 1 - 2 * (to % 2), sign, 0.0).astype(BF16)
    panel = jnp.concatenate([cols[:, 0].reshape(64, BLOCK), cols[:, 1].reshape(64, BLOCK)], 1)
    panel = panel * jnp.asarray(1.0 / N_FRAMES, BF16)
    right[:, :512] = panel
    right[:, 512:] = jnp.dot(swap, panel, preferred_element_type=F32).astype(BF16)

    copies = []
    for i in range(STRIPS):
        left = rows[:, i // 2, :, (i % 2) * STRIP : (i % 2 + 1) * STRIP].reshape(64, STRIP)
        product = lax.dot_general(
            left, right[...], (((0,), (0,)), ((), ())), preferred_element_type=F32
        )
        out[i, 0] = product[:, :512].astype(BF16)
        out[i, 1] = product[:, 512:].astype(BF16)
        copies.append(
            pltpu.make_async_copy(
                out.at[i], out_hbm.at[:, 0, pl.ds(i * STRIP, STRIP), :], sems.at[i]
            )
        )
        copies[-1].start()
    for copy in copies:
        copy.wait()


def local(samples, channel_index, gain_real, gain_imag, flags):
    in_hbm = pl.BlockSpec(memory_space=pltpu.HBM)
    vmem = pl.BlockSpec(memory_space=pltpu.VMEM)
    rows, cols = pl.pallas_call(
        gather_kernel,
        out_shape=(
            jax.ShapeDtypeStruct((N_FRAMES, 4, 2, BLOCK), BF16),
            jax.ShapeDtypeStruct((N_FRAMES, 2, 2, BLOCK), BF16),
        ),
        in_specs=[in_hbm] * 6,
        out_specs=(vmem, vmem),
        scratch_shapes=[
            pltpu.VMEM((P_SIZE, BLOCK), BF16),
            pltpu.SMEM((CHANNELS,), jnp.int32),
            pltpu.VMEM((TAPS, P_SIZE), F32),
            pltpu.VMEM((CHANNELS, BLOCK), F32),
            pltpu.VMEM((CHANNELS, BLOCK), F32),
            pltpu.VMEM((1, 128), jnp.int32),
            pltpu.VMEM((256, P_SIZE), BF16),
            pltpu.VMEM((CHANNELS * TAPS, 2, BLOCK), F32),
            pltpu.VMEM((TAPS, N_CHAN, 2, BLOCK), F32),
            pltpu.VMEM((N_CHAN, 2, BLOCK), BF16),
            pltpu.SemaphoreType.DMA((6,)),
            pltpu.SemaphoreType.DMA((TAPS,)),
            pltpu.SemaphoreType.DMA((2,)),
            pltpu.SemaphoreType.DMA((TAPS,)),
            pltpu.SemaphoreType.DMA,
            pltpu.SemaphoreType.DMA,
        ],
        compiler_params=pltpu.CompilerParams(
            collective_id=0, has_side_effects=True, vmem_limit_bytes=16 * 2**20
        ),
        name="spectra_and_gather",
    )(*[
        pltpu.with_memory_space_constraint(value, pltpu.HBM)
        for value in (samples, channel_index, jnp.asarray(filter_taps()), gain_real, gain_imag,
                      flags.reshape(1, 128))
    ])
    return pl.pallas_call(
        correlate_kernel,
        out_shape=jax.ShapeDtypeStruct((2, 1, 1024, 512), BF16),
        in_specs=[vmem, vmem],
        out_specs=pl.BlockSpec(memory_space=pltpu.HBM),
        scratch_shapes=[
            pltpu.VMEM((64, 1024), BF16),
            pltpu.VMEM((STRIPS, 2, STRIP, 512), BF16),
            pltpu.SemaphoreType.DMA((STRIPS,)),
        ],
        compiler_params=pltpu.CompilerParams(vmem_limit_bytes=16 * 2**20),
        name="correlate",
    )(rows, cols)


def solution(mesh):
    in_specs = (P(("tm", "row"), None, "chan"), P(), P(None, "chan"), P(None, "chan"), P("chan"))
    out_specs = P(None, "chan", "row", "tm")
    return jax.shard_map(local, mesh=mesh, in_specs=in_specs, out_specs=out_specs, check_vma=False)
```

```python
import functools
import math

import jax
import jax.numpy as jnp
import numpy as np
from jax import lax
from jax.experimental import pallas as pl
from jax.experimental.pallas import tpu as pltpu
from jax.sharding import PartitionSpec as P

P_SIZE = 4096
TAPS = 4
CHANNELS = 16
N_CHAN, N_TM, N_ROW = 16, 8, 4
N_FRAMES = N_TM * N_ROW
BLOCK = 256
CHUNK = 512
STRIP, STRIPS = 128, 8
MESH = pl.DeviceIdType.MESH
F32, BF16 = jnp.float32, jnp.bfloat16


def filter_taps():
    at = np.arange(TAPS * P_SIZE, dtype=np.float64) + 0.5
    centered = (at - TAPS * P_SIZE / 2) / P_SIZE
    taper = 0.5 - 0.5 * np.cos(2.0 * math.pi * at / (TAPS * P_SIZE))
    return (np.sinc(centered) * taper).reshape(TAPS, P_SIZE).astype(np.float32)


def cos_sin(phase):
    quarter = lax.shift_right_logical(phase + 512, 10)
    rest = phase - lax.shift_left(quarter, 10)
    x = rest.astype(F32) * (2.0 * math.pi / P_SIZE)
    y = x * x
    s = x + x * y * (-1 / 6 + y * (1 / 120 + y * (-1 / 5040 + y * (1 / 362880))))
    c = 1.0 + y * (-0.5 + y * (1 / 24 + y * (-1 / 720 + y * (1 / 40320))))
    odd = (quarter & 1) == 1
    cos = jnp.where(odd, s, c)
    sin = jnp.where(odd, c, s)
    cos = jnp.where(((quarter + 1) & 2) == 2, -cos, cos)
    sin = jnp.where((quarter & 2) == 2, -sin, sin)
    return cos, sin


FAR_FIRST = (4, 3, 5, 2, 6, 1, 7, 0)


def gather_kernel(
    x_hbm, ci_hbm, filt_hbm, gr_hbm, gi_hbm, flags_hbm,
    rows_out, cols_out,
    x, ci, filt, gr, gi, flags, lhs, send, parts, volts,
    local_sems, send_sem1, send_sem2, parts_sems, volts_sems,
):
    me_c = lax.axis_index("chan")
    me_t = lax.axis_index("tm")
    me_r = lax.axis_index("row")
    frame = me_t * N_ROW + me_r
    me_z = lax.rem(me_c, 8)
    me_half = lax.div(me_c, 8)
    rows_half = lax.div(me_r, 2)
    cols_half = lax.div(me_t, 4)
    ahead_count = jnp.minimum(N_FRAMES - 1 - frame, TAPS - 1)
    rows_count = N_FRAMES - jnp.where(rows_half == me_half, 1, 0)
    cols_count = N_FRAMES - jnp.where(cols_half == me_half, 1, 0)

    def place(number):
        return lax.div(number, N_ROW), lax.rem(number, N_ROW)

    barrier = pltpu.get_barrier_semaphore()

    def greet(c, at):
        pl.semaphore_signal(barrier, inc=1, device_id=(c, *at), device_id_type=MESH)

    line = [me_half * 8 + lax.rem(me_z + step, 8) for step in FAR_FIRST]
    for back in range(TAPS - 1, 0, -1):
        @pl.when(frame >= back)
        def _():
            for c in line:
                greet(c, place(frame - back))

    for c in line[:-1]:
        greet(c, (me_t, me_r))
    rows_from = rows_half * 8 + me_z
    cols_from = cols_half * 8 + me_z
    for step in sorted(range(1, N_FRAMES), key=lambda j: abs(j - N_FRAMES // 2)):
        at = place(lax.rem(frame + step, N_FRAMES))
        greet(rows_from, at)
        greet(cols_from, at)
    for source in (rows_from, cols_from):
        @pl.when(source != me_c)
        def _():
            greet(source, (me_t, me_r))

    loads = [
        pltpu.make_async_copy(src, dst, local_sems.at[i])
        for i, (src, dst) in enumerate(
            [(ci_hbm, ci), (filt_hbm, filt), (gr_hbm, gr), (gi_hbm, gi),
             (flags_hbm, flags), (x_hbm.at[0], x)]
        )
    ]
    for copy in loads:
        copy.start()

    for before in range(1, TAPS):
        @pl.when(frame < before)
        def _():
            parts[TAPS - 1 - before] = jnp.zeros(parts.shape[1:], F32)

    loads[0].wait()
    loads[1].wait()
    row_of = lax.broadcasted_iota(jnp.int32, (CHANNELS, CHUNK), 0)
    chan_at = jnp.zeros((CHANNELS, CHUNK), jnp.int32)
    for c in range(CHANNELS):
        chan_at = jnp.where(row_of == c, ci[c], chan_at)
    lane = lax.broadcasted_iota(jnp.int32, (CHANNELS, CHUNK), 1)

    def one_chunk(n, _):
        at = pl.ds(pl.multiple_of(n * CHUNK, CHUNK), CHUNK)
        phase = (chan_at * (lane + n * CHUNK)) & (P_SIZE - 1)
        cos, sin = cos_sin(phase)
        scale = 1.0 / math.sqrt(P_SIZE)
        table = (cos * scale, sin * -scale)
        for k in range(TAPS):
            tap = filt[k : k + 1, at]
            for part in range(2):
                value = table[part] * tap
                high = value.astype(BF16)
                low = (value - high.astype(F32)).astype(BF16)
                row = (2 * k + part) * CHANNELS
                lhs[row : row + CHANNELS, at] = high
                lhs[row + 128 : row + 128 + CHANNELS, at] = low
        return 0

    lax.fori_loop(0, P_SIZE // CHUNK, one_chunk, 0)

    for copy in loads[2:]:
        copy.wait()
    both = jnp.dot(lhs[...], x[...], preferred_element_type=F32)
    spectra = both[:128] + both[128:]

    twice = (
        lax.broadcasted_iota(jnp.int32, (128, BLOCK), 1) // 2
        == lax.broadcasted_iota(jnp.int32, (128, BLOCK), 0)
    ).astype(BF16)
    alive = jnp.dot(
        jnp.broadcast_to(flags[...].astype(F32), (CHANNELS, 128)).astype(BF16), twice,
        preferred_element_type=F32,
    )
    real_gain = gr[...] * alive
    imag_gain = gi[...] * alive
    planes = []
    for k in range(TAPS):
        s_re = spectra[32 * k : 32 * k + 16]
        s_im = spectra[32 * k + 16 : 32 * k + 32]
        planes += [real_gain * s_re - imag_gain * s_im, real_gain * s_im + imag_gain * s_re]
    planes = jnp.concatenate(planes, 0)
    to = lax.broadcasted_iota(jnp.int32, (128, 128), 0)
    source = ((to // 4 % 4) * 2 + to % 2) * 16 + (to // 2 % 2) * 8 + to // 16
    turn = (lax.broadcasted_iota(jnp.int32, (128, 128), 1) == source).astype(F32)
    turned = jnp.dot(
        turn, planes, precision=lax.Precision.HIGHEST, preferred_element_type=F32
    )
    send[...] = turned.reshape(32, 2, 2, BLOCK)

    pl.semaphore_wait(barrier, 8 * (1 + ahead_count) - 1 + rows_count + cols_count)

    def send_part(z, ahead):
        k = TAPS - 1 - ahead
        pltpu.make_async_remote_copy(
            src_ref=send.at[z * TAPS + k],
            dst_ref=parts.at[k, me_z],
            send_sem=send_sem1.at[k],
            recv_sem=parts_sems.at[k],
            device_id=(me_half * 8 + z, *place(frame + ahead)),
            device_id_type=MESH,
        ).start()

    for z in range(8):
        for ahead in range(TAPS - 1, 0, -1):
            @pl.when(frame + ahead < N_FRAMES)
            def _():
                send_part(z, ahead)

        @pl.when(me_z != z)
        def _():
            send_part(z, 0)
    parts[TAPS - 1, me_z] = send[me_z * TAPS + TAPS - 1]

    def wait_bytes(ref, sem):
        pltpu.make_async_copy(ref, ref, sem).wait()

    for k in range(TAPS - 1):
        @pl.when(frame >= TAPS - 1 - k)
        def _():
            wait_bytes(parts.at[k], parts_sems.at[k])
    wait_bytes(parts.at[TAPS - 1, pl.ds(0, 7)], parts_sems.at[TAPS - 1])

    for half in range(2):
        total = parts[0, :, half] + parts[1, :, half] + parts[2, :, half] + parts[3, :, half]
        volts[half] = total.astype(BF16)

    def send_volts(half, first, count, out, at, t, r):
        @pl.when((me_c != half * 8 + me_z) | (frame != t * N_ROW + r))
        def _():
            pltpu.make_async_remote_copy(
                src_ref=volts.at[half, pl.ds(first, count)],
                dst_ref=out.at[frame],
                send_sem=send_sem2.at[at],
                recv_sem=volts_sems.at[at],
                device_id=(half * 8 + me_z, t, r),
                device_id_type=MESH,
            ).start()

    def send_rows(t):
        for half in range(2):
            for r in (1, 0):
                send_volts(half, 4 * r, 4, rows_out, 0, t, me_half * 2 + r)

    def send_cols(n):
        part = n + me_half * (3 - 2 * n)
        for half in range(2):
            for r in (1, 3, 2, 0):
                send_volts(half, 2 * part, 2, cols_out, 1, me_half * 4 + part, r)

    for n, t in enumerate((0, 1, 2, 7, 3, 6, 5, 4)):
        send_rows(t)
        if n == 1:
            for i in range(4):
                send_cols(i)

    @pl.when(rows_half == me_half)
    def _():
        rows_out[frame] = volts[me_half, pl.ds(4 * lax.rem(me_r, 2), 4)]

    @pl.when(cols_half == me_half)
    def _():
        cols_out[frame] = volts[me_half, pl.ds(2 * lax.rem(me_t, 4), 2)]

    for at, (ref, half) in enumerate(((rows_out, rows_half), (cols_out, cols_half))):
        for sems in (volts_sems, send_sem2):
            @pl.when(half == me_half)
            def _():
                wait_bytes(ref.at[pl.ds(0, N_FRAMES - 1)], sems.at[at])

            @pl.when(half != me_half)
            def _():
                wait_bytes(ref, sems.at[at])
    for k in range(TAPS - 1):
        @pl.when(frame + TAPS - 1 - k < N_FRAMES)
        def _():
            wait_bytes(parts.at[k], send_sem1.at[k])
    wait_bytes(parts.at[TAPS - 1, pl.ds(0, 7)], send_sem1.at[TAPS - 1])


def correlate_kernel(rows, cols, out_hbm, right, out, sems):
    to = lax.broadcasted_iota(jnp.int32, (64, 64), 0)
    at = lax.broadcasted_iota(jnp.int32, (64, 64), 1)
    sign = jnp.where(to % 2 == 0, -1.0, 1.0)
    swap = jnp.where(at == to + 1 - 2 * (to % 2), sign, 0.0).astype(BF16)
    panel = jnp.concatenate([cols[:, 0].reshape(64, BLOCK), cols[:, 1].reshape(64, BLOCK)], 1)
    panel = panel * jnp.asarray(1.0 / N_FRAMES, BF16)
    right[:, :512] = panel
    right[:, 512:] = jnp.dot(swap, panel, preferred_element_type=F32).astype(BF16)

    copies = []
    for i in range(STRIPS):
        left = rows[:, i // 2, :, (i % 2) * STRIP : (i % 2 + 1) * STRIP].reshape(64, STRIP)
        product = lax.dot_general(
            left, right[...], (((0,), (0,)), ((), ())), preferred_element_type=F32
        )
        out[i, 0] = product[:, :512].astype(BF16)
        out[i, 1] = product[:, 512:].astype(BF16)
        copies.append(
            pltpu.make_async_copy(
                out.at[i], out_hbm.at[:, 0, pl.ds(i * STRIP, STRIP), :], sems.at[i]
            )
        )
        copies[-1].start()
    for copy in copies:
        copy.wait()


def local(samples, channel_index, gain_real, gain_imag, flags):
    in_hbm = pl.BlockSpec(memory_space=pltpu.HBM)
    vmem = pl.BlockSpec(memory_space=pltpu.VMEM)
    rows, cols = pl.pallas_call(
        gather_kernel,
        out_shape=(
            jax.ShapeDtypeStruct((N_FRAMES, 4, 2, BLOCK), BF16),
            jax.ShapeDtypeStruct((N_FRAMES, 2, 2, BLOCK), BF16),
        ),
        in_specs=[in_hbm] * 6,
        out_specs=(vmem, vmem),
        scratch_shapes=[
            pltpu.VMEM((P_SIZE, BLOCK), BF16),
            pltpu.SMEM((CHANNELS,), jnp.int32),
            pltpu.VMEM((TAPS, P_SIZE), F32),
            pltpu.VMEM((CHANNELS, BLOCK), F32),
            pltpu.VMEM((CHANNELS, BLOCK), F32),
            pltpu.VMEM((1, 128), jnp.int32),
            pltpu.VMEM((256, P_SIZE), BF16),
            pltpu.VMEM((8 * TAPS, 2, 2, BLOCK), F32),
            pltpu.VMEM((TAPS, 8, 2, 2, BLOCK), F32),
            pltpu.VMEM((2, 8, 2, BLOCK), BF16),
            pltpu.SemaphoreType.DMA((6,)),
            pltpu.SemaphoreType.DMA((TAPS,)),
            pltpu.SemaphoreType.DMA((2,)),
            pltpu.SemaphoreType.DMA((TAPS,)),
            pltpu.SemaphoreType.DMA((2,)),
        ],
        compiler_params=pltpu.CompilerParams(
            collective_id=0, has_side_effects=True, vmem_limit_bytes=16 * 2**20
        ),
        name="spectra_and_gather",
    )(*[
        pltpu.with_memory_space_constraint(value, pltpu.HBM)
        for value in (samples, channel_index, jnp.asarray(filter_taps()), gain_real, gain_imag,
                      flags.reshape(1, 128))
    ])
    return pl.pallas_call(
        correlate_kernel,
        out_shape=jax.ShapeDtypeStruct((2, 1, 1024, 512), BF16),
        in_specs=[vmem, vmem],
        out_specs=pl.BlockSpec(memory_space=pltpu.HBM),
        scratch_shapes=[
            pltpu.VMEM((64, 1024), BF16),
            pltpu.VMEM((STRIPS, 2, STRIP, 512), BF16),
            pltpu.SemaphoreType.DMA((STRIPS,)),
        ],
        compiler_params=pltpu.CompilerParams(vmem_limit_bytes=16 * 2**20),
        name="correlate",
    )(rows, cols)


def solution(mesh):
    in_specs = (P(("tm", "row"), None, "chan"), P(), P(None, "chan"), P(None, "chan"), P("chan"))
    out_specs = P(None, "chan", "row", "tm")
    return jax.shard_map(local, mesh=mesh, in_specs=in_specs, out_specs=out_specs, check_vma=False)
```

```python
import functools
import math

import jax
import jax.numpy as jnp
import numpy as np
from jax import lax
from jax.experimental import pallas as pl
from jax.experimental.pallas import tpu as pltpu
from jax.sharding import PartitionSpec as P

P_SIZE = 4096
TAPS = 4
CHANNELS = 16
N_CHAN, N_TM, N_ROW = 16, 8, 4
N_FRAMES = N_TM * N_ROW
BLOCK = 256
CHUNK = 512
STRIP, STRIPS = 128, 8
MESH = pl.DeviceIdType.MESH
F32, BF16 = jnp.float32, jnp.bfloat16


def filter_taps():
    at = np.arange(TAPS * P_SIZE, dtype=np.float64) + 0.5
    centered = (at - TAPS * P_SIZE / 2) / P_SIZE
    taper = 0.5 - 0.5 * np.cos(2.0 * math.pi * at / (TAPS * P_SIZE))
    return (np.sinc(centered) * taper).reshape(TAPS, P_SIZE).astype(np.float32)


def cos_sin(phase):
    quarter = lax.shift_right_logical(phase + 512, 10)
    rest = phase - lax.shift_left(quarter, 10)
    x = rest.astype(F32) * (2.0 * math.pi / P_SIZE)
    y = x * x
    s = x + x * y * (-1 / 6 + y * (1 / 120 + y * (-1 / 5040 + y * (1 / 362880))))
    c = 1.0 + y * (-0.5 + y * (1 / 24 + y * (-1 / 720 + y * (1 / 40320))))
    odd = (quarter & 1) == 1
    cos = jnp.where(odd, s, c)
    sin = jnp.where(odd, c, s)
    cos = jnp.where(((quarter + 1) & 2) == 2, -cos, cos)
    sin = jnp.where((quarter & 2) == 2, -sin, sin)
    return cos, sin


FAR_FIRST = (4, 3, 5, 2, 6, 1, 7, 0)


def gather_kernel(
    x_hbm, ci_hbm, filt_hbm, gr_hbm, gi_hbm, flags_hbm,
    rows_out, right,
    x, ci, filt, gr, gi, flags, lhs, send, parts, volts, cols,
    local_sems, send_sem1, send_sem2, parts_sems, volts_sems,
):
    me_c = lax.axis_index("chan")
    me_t = lax.axis_index("tm")
    me_r = lax.axis_index("row")
    frame = me_t * N_ROW + me_r
    me_z = lax.rem(me_c, 8)
    me_half = lax.div(me_c, 8)
    rows_half = lax.div(me_r, 2)
    cols_half = lax.div(me_t, 4)
    ahead_count = jnp.minimum(N_FRAMES - 1 - frame, TAPS - 1)
    rows_count = N_FRAMES - jnp.where(rows_half == me_half, 1, 0)
    cols_count = N_FRAMES - jnp.where(cols_half == me_half, 1, 0)

    def place(number):
        return lax.div(number, N_ROW), lax.rem(number, N_ROW)

    barrier = pltpu.get_barrier_semaphore()

    def greet(c, at):
        pl.semaphore_signal(barrier, inc=1, device_id=(c, *at), device_id_type=MESH)

    line = [me_half * 8 + lax.rem(me_z + step, 8) for step in FAR_FIRST]
    rows_from = rows_half * 8 + me_z
    cols_from = cols_half * 8 + me_z
    for step in sorted(range(1, N_FRAMES), key=lambda j: abs(j - N_FRAMES // 2)):
        at = place(lax.rem(frame + step, N_FRAMES))
        greet(rows_from, at)
        greet(cols_from, at)
    for source in (rows_from, cols_from):
        @pl.when(source != me_c)
        def _():
            greet(source, (me_t, me_r))

    for back in range(TAPS - 1, 0, -1):
        @pl.when(frame >= back)
        def _():
            for c in line:
                greet(c, place(frame - back))

    for c in line[:-1]:
        greet(c, (me_t, me_r))

    loads = [
        pltpu.make_async_copy(src, dst, local_sems.at[i])
        for i, (src, dst) in enumerate(
            [(ci_hbm, ci), (filt_hbm, filt), (gr_hbm, gr), (gi_hbm, gi),
             (flags_hbm, flags), (x_hbm.at[0], x)]
        )
    ]
    for copy in loads:
        copy.start()

    for before in range(1, TAPS):
        @pl.when(frame < before)
        def _():
            parts[TAPS - 1 - before] = jnp.zeros(parts.shape[1:], F32)

    loads[0].wait()
    loads[1].wait()
    row_of = lax.broadcasted_iota(jnp.int32, (CHANNELS, CHUNK), 0)
    chan_at = jnp.zeros((CHANNELS, CHUNK), jnp.int32)
    for c in range(CHANNELS):
        chan_at = jnp.where(row_of == c, ci[c], chan_at)
    lane = lax.broadcasted_iota(jnp.int32, (CHANNELS, CHUNK), 1)

    def one_chunk(n, _):
        at = pl.ds(pl.multiple_of(n * CHUNK, CHUNK), CHUNK)
        phase = (chan_at * (lane + n * CHUNK)) & (P_SIZE - 1)
        cos, sin = cos_sin(phase)
        scale = 1.0 / math.sqrt(P_SIZE)
        table = (cos * scale, sin * -scale)
        for k in range(TAPS):
            tap = filt[k : k + 1, at]
            for part in range(2):
                value = table[part] * tap
                high = value.astype(BF16)
                low = (value - high.astype(F32)).astype(BF16)
                row = (2 * k + part) * CHANNELS
                lhs[row : row + CHANNELS, at] = high
                lhs[row + 128 : row + 128 + CHANNELS, at] = low
        return 0

    lax.fori_loop(0, P_SIZE // CHUNK, one_chunk, 0)

    for copy in loads[2:]:
        copy.wait()
    both = jnp.dot(lhs[...], x[...], preferred_element_type=F32)
    spectra = both[:128] + both[128:]

    twice = (
        lax.broadcasted_iota(jnp.int32, (128, BLOCK), 1) // 2
        == lax.broadcasted_iota(jnp.int32, (128, BLOCK), 0)
    ).astype(BF16)
    alive = jnp.dot(
        jnp.broadcast_to(flags[...].astype(F32), (CHANNELS, 128)).astype(BF16), twice,
        preferred_element_type=F32,
    )
    real_gain = gr[...] * alive
    imag_gain = gi[...] * alive
    planes = []
    for k in range(TAPS):
        s_re = spectra[32 * k : 32 * k + 16]
        s_im = spectra[32 * k + 16 : 32 * k + 32]
        planes += [real_gain * s_re - imag_gain * s_im, real_gain * s_im + imag_gain * s_re]
    planes = jnp.concatenate(planes, 0)
    to = lax.broadcasted_iota(jnp.int32, (128, 128), 0)
    source = ((to // 4 % 4) * 2 + to % 2) * 16 + (to // 2 % 2) * 8 + to // 16
    turn = (lax.broadcasted_iota(jnp.int32, (128, 128), 1) == source).astype(F32)
    turned = jnp.dot(
        turn, planes, precision=lax.Precision.HIGHEST, preferred_element_type=F32
    )
    send[...] = turned.reshape(32, 2, 2, BLOCK)

    pl.semaphore_wait(barrier, 8 * (1 + ahead_count) - 1 + rows_count + cols_count)

    def send_part(z, ahead):
        k = TAPS - 1 - ahead
        pltpu.make_async_remote_copy(
            src_ref=send.at[z * TAPS + k],
            dst_ref=parts.at[k, me_z],
            send_sem=send_sem1.at[k],
            recv_sem=parts_sems.at[k],
            device_id=(me_half * 8 + z, *place(frame + ahead)),
            device_id_type=MESH,
        ).start()

    for z in range(8):
        for ahead in range(TAPS - 1, 0, -1):
            @pl.when(frame + ahead < N_FRAMES)
            def _():
                send_part(z, ahead)

        @pl.when(me_z != z)
        def _():
            send_part(z, 0)
    parts[TAPS - 1, me_z] = send[me_z * TAPS + TAPS - 1]

    def wait_bytes(ref, sem):
        pltpu.make_async_copy(ref, ref, sem).wait()

    for k in range(TAPS - 1):
        @pl.when(frame >= TAPS - 1 - k)
        def _():
            wait_bytes(parts.at[k], parts_sems.at[k])
    wait_bytes(parts.at[TAPS - 1, pl.ds(0, 7)], parts_sems.at[TAPS - 1])

    for half in range(2):
        total = parts[0, :, half] + parts[1, :, half] + parts[2, :, half] + parts[3, :, half]
        volts[half] = total.astype(BF16)

    def send_volts(half, first, count, out, at, t, r):
        @pl.when((me_c != half * 8 + me_z) | (frame != t * N_ROW + r))
        def _():
            pltpu.make_async_remote_copy(
                src_ref=volts.at[half, pl.ds(first, count)],
                dst_ref=out.at[frame],
                send_sem=send_sem2.at[at],
                recv_sem=volts_sems.at[at],
                device_id=(half * 8 + me_z, t, r),
                device_id_type=MESH,
            ).start()

    def send_rows(t):
        for half in range(2):
            for r in (1, 0):
                send_volts(half, 4 * r, 4, rows_out, 0, t, me_half * 2 + r)

    def send_cols(n):
        part = n + me_half * (3 - 2 * n)
        for half in range(2):
            for r in (1, 3, 2, 0):
                send_volts(half, 2 * part, 2, cols, 1, me_half * 4 + part, r)

    for t in (0, 1):
        send_rows(t)
    for n in range(4):
        send_cols(n)
    for step in FAR_FIRST:
        t = lax.rem(me_t + step, N_TM)

        @pl.when((t != 0) & (t != 1))
        def _():
            send_rows(t)

    @pl.when(rows_half == me_half)
    def _():
        rows_out[frame] = volts[me_half, pl.ds(4 * lax.rem(me_r, 2), 4)]

    @pl.when(cols_half == me_half)
    def _():
        cols[frame] = volts[me_half, pl.ds(2 * lax.rem(me_t, 4), 2)]

    def wait_volts(ref, half, sem):
        @pl.when(half == me_half)
        def _():
            wait_bytes(ref.at[pl.ds(0, N_FRAMES - 1)], sem)

        @pl.when(half != me_half)
        def _():
            wait_bytes(ref, sem)

    wait_volts(cols, cols_half, volts_sems.at[1])
    to = lax.broadcasted_iota(jnp.int32, (64, 64), 0)
    at = lax.broadcasted_iota(jnp.int32, (64, 64), 1)
    sign = jnp.where(to % 2 == 0, -1.0, 1.0)
    swap = jnp.where(at == to + 1 - 2 * (to % 2), sign, 0.0).astype(BF16)
    panel = jnp.concatenate([cols[:, 0].reshape(64, BLOCK), cols[:, 1].reshape(64, BLOCK)], 1)
    panel = panel * jnp.asarray(1.0 / N_FRAMES, BF16)
    right[:, :512] = panel
    right[:, 512:] = jnp.dot(swap, panel, preferred_element_type=F32).astype(BF16)

    wait_volts(rows_out, rows_half, volts_sems.at[0])
    wait_volts(rows_out, rows_half, send_sem2.at[0])
    wait_volts(cols, cols_half, send_sem2.at[1])
    for k in range(TAPS - 1):
        @pl.when(frame + TAPS - 1 - k < N_FRAMES)
        def _():
            wait_bytes(parts.at[k], send_sem1.at[k])
    wait_bytes(parts.at[TAPS - 1, pl.ds(0, 7)], send_sem1.at[TAPS - 1])


def correlate_kernel(rows, right, out_hbm, out, sems):
    copies = []
    for i in range(STRIPS):
        left = rows[:, i // 2, :, (i % 2) * STRIP : (i % 2 + 1) * STRIP].reshape(64, STRIP)
        product = lax.dot_general(
            left, right[...], (((0,), (0,)), ((), ())), preferred_element_type=F32
        )
        out[i, 0] = product[:, :512].astype(BF16)
        out[i, 1] = product[:, 512:].astype(BF16)
        copies.append(
            pltpu.make_async_copy(
                out.at[i], out_hbm.at[:, 0, pl.ds(i * STRIP, STRIP), :], sems.at[i]
            )
        )
        copies[-1].start()
    for copy in copies:
        copy.wait()


def local(samples, channel_index, gain_real, gain_imag, flags):
    in_hbm = pl.BlockSpec(memory_space=pltpu.HBM)
    vmem = pl.BlockSpec(memory_space=pltpu.VMEM)
    rows, right = pl.pallas_call(
        gather_kernel,
        out_shape=(
            jax.ShapeDtypeStruct((N_FRAMES, 4, 2, BLOCK), BF16),
            jax.ShapeDtypeStruct((64, 1024), BF16),
        ),
        in_specs=[in_hbm] * 6,
        out_specs=(vmem, vmem),
        scratch_shapes=[
            pltpu.VMEM((P_SIZE, BLOCK), BF16),
            pltpu.SMEM((CHANNELS,), jnp.int32),
            pltpu.VMEM((TAPS, P_SIZE), F32),
            pltpu.VMEM((CHANNELS, BLOCK), F32),
            pltpu.VMEM((CHANNELS, BLOCK), F32),
            pltpu.VMEM((1, 128), jnp.int32),
            pltpu.VMEM((256, P_SIZE), BF16),
            pltpu.VMEM((8 * TAPS, 2, 2, BLOCK), F32),
            pltpu.VMEM((TAPS, 8, 2, 2, BLOCK), F32),
            pltpu.VMEM((2, 8, 2, BLOCK), BF16),
            pltpu.VMEM((N_FRAMES, 2, 2, BLOCK), BF16),
            pltpu.SemaphoreType.DMA((6,)),
            pltpu.SemaphoreType.DMA((TAPS,)),
            pltpu.SemaphoreType.DMA((2,)),
            pltpu.SemaphoreType.DMA((TAPS,)),
            pltpu.SemaphoreType.DMA((2,)),
        ],
        compiler_params=pltpu.CompilerParams(
            collective_id=0, has_side_effects=True, vmem_limit_bytes=16 * 2**20
        ),
        name="spectra_and_gather",
    )(*[
        pltpu.with_memory_space_constraint(value, pltpu.HBM)
        for value in (samples, channel_index, jnp.asarray(filter_taps()), gain_real, gain_imag,
                      flags.reshape(1, 128))
    ])
    return pl.pallas_call(
        correlate_kernel,
        out_shape=jax.ShapeDtypeStruct((2, 1, 1024, 512), BF16),
        in_specs=[vmem, vmem],
        out_specs=pl.BlockSpec(memory_space=pltpu.HBM),
        scratch_shapes=[
            pltpu.VMEM((STRIPS, 2, STRIP, 512), BF16),
            pltpu.SemaphoreType.DMA((STRIPS,)),
        ],
        compiler_params=pltpu.CompilerParams(vmem_limit_bytes=16 * 2**20),
        name="correlate",
    )(rows, right)


def solution(mesh):
    in_specs = (P(("tm", "row"), None, "chan"), P(), P(None, "chan"), P(None, "chan"), P("chan"))
    out_specs = P(None, "chan", "row", "tm")
    return jax.shard_map(local, mesh=mesh, in_specs=in_specs, out_specs=out_specs, check_vma=False)
```

```python
import functools
import math

import jax
import jax.numpy as jnp
import numpy as np
from jax import lax
from jax.experimental import pallas as pl
from jax.experimental.pallas import tpu as pltpu
from jax.sharding import PartitionSpec as P

P_SIZE = 4096
TAPS = 4
CHANNELS = 16
N_CHAN, N_TM, N_ROW = 16, 8, 4
N_FRAMES = N_TM * N_ROW
BLOCK = 256
CHUNK = 512
STRIP, STRIPS = 128, 8
MESH = pl.DeviceIdType.MESH
F32, BF16 = jnp.float32, jnp.bfloat16


def filter_taps():
    at = np.arange(TAPS * P_SIZE, dtype=np.float64) + 0.5
    centered = (at - TAPS * P_SIZE / 2) / P_SIZE
    taper = 0.5 - 0.5 * np.cos(2.0 * math.pi * at / (TAPS * P_SIZE))
    return (np.sinc(centered) * taper).reshape(TAPS, P_SIZE).astype(np.float32)


def cos_sin(phase):
    quarter = lax.shift_right_logical(phase + 512, 10)
    rest = phase - lax.shift_left(quarter, 10)
    x = rest.astype(F32) * (2.0 * math.pi / P_SIZE)
    y = x * x
    s = x + x * y * (-1 / 6 + y * (1 / 120 + y * (-1 / 5040 + y * (1 / 362880))))
    c = 1.0 + y * (-0.5 + y * (1 / 24 + y * (-1 / 720 + y * (1 / 40320))))
    odd = (quarter & 1) == 1
    cos = jnp.where(odd, s, c)
    sin = jnp.where(odd, c, s)
    cos = jnp.where(((quarter + 1) & 2) == 2, -cos, cos)
    sin = jnp.where((quarter & 2) == 2, -sin, sin)
    return cos, sin


FAR_FIRST = (4, 3, 5, 2, 6, 1, 7, 0)


def gather_kernel(
    x_hbm, ci_hbm, filt_hbm, gr_hbm, gi_hbm, flags_hbm,
    rows_out, right,
    x, ci, filt, gr, gi, flags, lhs, send, parts, volts, cols,
    local_sems, send_sem1, send_sem2, parts_sems, volts_sems,
):
    me_c = lax.axis_index("chan")
    me_t = lax.axis_index("tm")
    me_r = lax.axis_index("row")
    frame = me_t * N_ROW + me_r
    me_z = lax.rem(me_c, 8)
    me_half = lax.div(me_c, 8)
    rows_half = lax.div(me_r, 2)
    cols_half = lax.div(me_t, 4)
    ahead_count = jnp.minimum(N_FRAMES - 1 - frame, TAPS - 1)
    rows_count = N_FRAMES - jnp.where(rows_half == me_half, 1, 0)
    cols_count = N_FRAMES - jnp.where(cols_half == me_half, 1, 0)

    def place(number):
        return lax.div(number, N_ROW), lax.rem(number, N_ROW)

    barrier = pltpu.get_barrier_semaphore()

    def greet(c, at):
        pl.semaphore_signal(barrier, inc=1, device_id=(c, *at), device_id_type=MESH)

    line = [me_half * 8 + lax.rem(me_z + step, 8) for step in FAR_FIRST]
    rows_from = rows_half * 8 + me_z
    cols_from = cols_half * 8 + me_z
    for step in sorted(range(1, N_FRAMES), key=lambda j: abs(j - N_FRAMES // 2)):
        at = place(lax.rem(frame + step, N_FRAMES))
        greet(rows_from, at)
        greet(cols_from, at)
    for source in (rows_from, cols_from):
        @pl.when(source != me_c)
        def _():
            greet(source, (me_t, me_r))

    for back in range(TAPS - 1, 0, -1):
        @pl.when(frame >= back)
        def _():
            for c in line:
                greet(c, place(frame - back))

    for c in line[:-1]:
        greet(c, (me_t, me_r))

    loads = [
        pltpu.make_async_copy(src, dst, local_sems.at[i])
        for i, (src, dst) in enumerate(
            [(ci_hbm, ci), (filt_hbm, filt), (gr_hbm, gr), (gi_hbm, gi),
             (flags_hbm, flags), (x_hbm.at[0], x)]
        )
    ]
    for copy in loads:
        copy.start()

    for before in range(1, TAPS):
        @pl.when(frame < before)
        def _():
            parts[TAPS - 1 - before] = jnp.zeros(parts.shape[1:], F32)

    loads[0].wait()
    loads[1].wait()
    row_of = lax.broadcasted_iota(jnp.int32, (CHANNELS, CHUNK), 0)
    chan_at = jnp.zeros((CHANNELS, CHUNK), jnp.int32)
    for c in range(CHANNELS):
        chan_at = jnp.where(row_of == c, ci[c], chan_at)
    lane = lax.broadcasted_iota(jnp.int32, (CHANNELS, CHUNK), 1)

    def one_chunk(n, _):
        at = pl.ds(pl.multiple_of(n * CHUNK, CHUNK), CHUNK)
        phase = (chan_at * (lane + n * CHUNK)) & (P_SIZE - 1)
        cos, sin = cos_sin(phase)
        scale = 1.0 / math.sqrt(P_SIZE)
        table = (cos * scale, sin * -scale)
        for k in range(TAPS):
            tap = filt[k : k + 1, at]
            for part in range(2):
                value = table[part] * tap
                high = value.astype(BF16)
                low = (value - high.astype(F32)).astype(BF16)
                row = (2 * k + part) * CHANNELS
                lhs[row : row + CHANNELS, at] = high
                lhs[row + 128 : row + 128 + CHANNELS, at] = low
        return 0

    lax.fori_loop(0, P_SIZE // CHUNK, one_chunk, 0)

    for copy in loads[2:]:
        copy.wait()
    both = jnp.dot(lhs[...], x[...], preferred_element_type=F32)
    spectra = both[:128] + both[128:]

    twice = (
        lax.broadcasted_iota(jnp.int32, (128, BLOCK), 1) // 2
        == lax.broadcasted_iota(jnp.int32, (128, BLOCK), 0)
    ).astype(BF16)
    alive = jnp.dot(
        jnp.broadcast_to(flags[...].astype(F32), (CHANNELS, 128)).astype(BF16), twice,
        preferred_element_type=F32,
    )
    real_gain = gr[...] * alive
    imag_gain = gi[...] * alive
    planes = []
    for k in range(TAPS):
        s_re = spectra[32 * k : 32 * k + 16]
        s_im = spectra[32 * k + 16 : 32 * k + 32]
        planes += [real_gain * s_re - imag_gain * s_im, real_gain * s_im + imag_gain * s_re]
    planes = jnp.concatenate(planes, 0)
    to = lax.broadcasted_iota(jnp.int32, (128, 128), 0)
    source = ((to // 4 % 4) * 2 + to % 2) * 16 + (to // 2 % 2) * 8 + to // 16
    turn = (lax.broadcasted_iota(jnp.int32, (128, 128), 1) == source).astype(F32)
    turned = jnp.dot(
        turn, planes, precision=lax.Precision.HIGHEST, preferred_element_type=F32
    )
    send[...] = turned.reshape(32, 2, 2, BLOCK)

    pl.semaphore_wait(barrier, 8 * (1 + ahead_count) - 1 + rows_count + cols_count)

    def send_part(z, ahead):
        k = TAPS - 1 - ahead
        pltpu.make_async_remote_copy(
            src_ref=send.at[z * TAPS + k],
            dst_ref=parts.at[k, me_z],
            send_sem=send_sem1.at[k],
            recv_sem=parts_sems.at[k],
            device_id=(me_half * 8 + z, *place(frame + ahead)),
            device_id_type=MESH,
        ).start()

    for z in range(8):
        for ahead in range(TAPS - 1, 0, -1):
            @pl.when(frame + ahead < N_FRAMES)
            def _():
                send_part(z, ahead)

        @pl.when(me_z != z)
        def _():
            send_part(z, 0)
    parts[TAPS - 1, me_z] = send[me_z * TAPS + TAPS - 1]

    def wait_bytes(ref, sem):
        pltpu.make_async_copy(ref, ref, sem).wait()

    for k in range(TAPS - 1):
        @pl.when(frame >= TAPS - 1 - k)
        def _():
            wait_bytes(parts.at[k], parts_sems.at[k])
    wait_bytes(parts.at[TAPS - 1, pl.ds(0, 7)], parts_sems.at[TAPS - 1])

    for half in range(2):
        total = parts[0, :, half] + parts[1, :, half] + parts[2, :, half] + parts[3, :, half]
        volts[half] = total.astype(BF16)

    def send_volts(half, first, count, out, at, t, r):
        @pl.when((me_c != half * 8 + me_z) | (frame != t * N_ROW + r))
        def _():
            pltpu.make_async_remote_copy(
                src_ref=volts.at[half, pl.ds(first, count)],
                dst_ref=out.at[frame],
                send_sem=send_sem2.at[at],
                recv_sem=volts_sems.at[at],
                device_id=(half * 8 + me_z, t, r),
                device_id_type=MESH,
            ).start()

    def send_rows(t):
        for half in range(2):
            for r in (1, 0):
                send_volts(half, 4 * r, 4, rows_out, 0, t, me_half * 2 + r)

    def send_cols(n):
        part = n + me_half * (3 - 2 * n)
        for half in range(2):
            for r in (1, 3, 2, 0):
                send_volts(half, 2 * part, 2, cols, 1, me_half * 4 + part, r)

    for n, t in enumerate((0, 1, 2, 7, 3, 6, 5, 4)):
        send_rows(t)
        if n == 1:
            for i in range(4):
                send_cols(i)

    @pl.when(rows_half == me_half)
    def _():
        rows_out[frame] = volts[me_half, pl.ds(4 * lax.rem(me_r, 2), 4)]

    @pl.when(cols_half == me_half)
    def _():
        cols[frame] = volts[me_half, pl.ds(2 * lax.rem(me_t, 4), 2)]

    def wait_volts(ref, half, sem):
        @pl.when(half == me_half)
        def _():
            wait_bytes(ref.at[pl.ds(0, N_FRAMES - 1)], sem)

        @pl.when(half != me_half)
        def _():
            wait_bytes(ref, sem)

    wait_volts(cols, cols_half, volts_sems.at[1])
    to = lax.broadcasted_iota(jnp.int32, (64, 64), 0)
    at = lax.broadcasted_iota(jnp.int32, (64, 64), 1)
    sign = jnp.where(to % 2 == 0, -1.0, 1.0)
    swap = jnp.where(at == to + 1 - 2 * (to % 2), sign, 0.0).astype(BF16)
    panel = jnp.concatenate([cols[:, 0].reshape(64, BLOCK), cols[:, 1].reshape(64, BLOCK)], 1)
    panel = panel * jnp.asarray(1.0 / N_FRAMES, BF16)
    right[:, :512] = panel
    right[:, 512:] = jnp.dot(swap, panel, preferred_element_type=F32).astype(BF16)

    wait_volts(rows_out, rows_half, volts_sems.at[0])
    wait_volts(rows_out, rows_half, send_sem2.at[0])
    wait_volts(cols, cols_half, send_sem2.at[1])
    for k in range(TAPS - 1):
        @pl.when(frame + TAPS - 1 - k < N_FRAMES)
        def _():
            wait_bytes(parts.at[k], send_sem1.at[k])
    wait_bytes(parts.at[TAPS - 1, pl.ds(0, 7)], send_sem1.at[TAPS - 1])


def correlate_kernel(rows, right, out_hbm, out, sems):
    copies = []
    for i in range(STRIPS):
        left = rows[:, i // 2, :, (i % 2) * STRIP : (i % 2 + 1) * STRIP].reshape(64, STRIP)
        product = lax.dot_general(
            left, right[...], (((0,), (0,)), ((), ())), preferred_element_type=F32
        )
        out[i, 0] = product[:, :512].astype(BF16)
        out[i, 1] = product[:, 512:].astype(BF16)
        copies.append(
            pltpu.make_async_copy(
                out.at[i], out_hbm.at[:, 0, pl.ds(i * STRIP, STRIP), :], sems.at[i]
            )
        )
        copies[-1].start()
    for copy in copies:
        copy.wait()


def local(samples, channel_index, gain_real, gain_imag, flags):
    in_hbm = pl.BlockSpec(memory_space=pltpu.HBM)
    vmem = pl.BlockSpec(memory_space=pltpu.VMEM)
    rows, right = pl.pallas_call(
        gather_kernel,
        out_shape=(
            jax.ShapeDtypeStruct((N_FRAMES, 4, 2, BLOCK), BF16),
            jax.ShapeDtypeStruct((64, 1024), BF16),
        ),
        in_specs=[in_hbm] * 6,
        out_specs=(vmem, vmem),
        scratch_shapes=[
            pltpu.VMEM((P_SIZE, BLOCK), BF16),
            pltpu.SMEM((CHANNELS,), jnp.int32),
            pltpu.VMEM((TAPS, P_SIZE), F32),
            pltpu.VMEM((CHANNELS, BLOCK), F32),
            pltpu.VMEM((CHANNELS, BLOCK), F32),
            pltpu.VMEM((1, 128), jnp.int32),
            pltpu.VMEM((256, P_SIZE), BF16),
            pltpu.VMEM((8 * TAPS, 2, 2, BLOCK), F32),
            pltpu.VMEM((TAPS, 8, 2, 2, BLOCK), F32),
            pltpu.VMEM((2, 8, 2, BLOCK), BF16),
            pltpu.VMEM((N_FRAMES, 2, 2, BLOCK), BF16),
            pltpu.SemaphoreType.DMA((6,)),
            pltpu.SemaphoreType.DMA((TAPS,)),
            pltpu.SemaphoreType.DMA((2,)),
            pltpu.SemaphoreType.DMA((TAPS,)),
            pltpu.SemaphoreType.DMA((2,)),
        ],
        compiler_params=pltpu.CompilerParams(
            collective_id=0, has_side_effects=True, vmem_limit_bytes=16 * 2**20
        ),
        name="spectra_and_gather",
    )(*[
        pltpu.with_memory_space_constraint(value, pltpu.HBM)
        for value in (samples, channel_index, jnp.asarray(filter_taps()), gain_real, gain_imag,
                      flags.reshape(1, 128))
    ])
    return pl.pallas_call(
        correlate_kernel,
        out_shape=jax.ShapeDtypeStruct((2, 1, 1024, 512), BF16),
        in_specs=[vmem, vmem],
        out_specs=pl.BlockSpec(memory_space=pltpu.HBM),
        scratch_shapes=[
            pltpu.VMEM((STRIPS, 2, STRIP, 512), BF16),
            pltpu.SemaphoreType.DMA((STRIPS,)),
        ],
        compiler_params=pltpu.CompilerParams(vmem_limit_bytes=16 * 2**20),
        name="correlate",
    )(rows, right)


def solution(mesh):
    in_specs = (P(("tm", "row"), None, "chan"), P(), P(None, "chan"), P(None, "chan"), P("chan"))
    out_specs = P(None, "chan", "row", "tm")
    return jax.shard_map(local, mesh=mesh, in_specs=in_specs, out_specs=out_specs, check_vma=False)
```
